256 devices in a mesh: grp: 4 (over x), row: 64 (over y, z, core).
Axes of the slice: x: 4, y: 4, z: 8, core: 2. Of those that a mesh axis runs over, the one named last changes fastest.
Arguments:
- snapshots: float32 [229376, 2048], P('row', 'grp'), may hold values from -24 to 24, as said below
- test_block: float32 [229376, 512], P('row', 'grp'), may hold values from -24 to 24, as said below
- start_block: float32 [2048, 64], P('grp'), may hold values from -6 to 6
- start_merge: float32 [256, 64], replicated, may hold values from -6 to 6
Outputs:
- projected: float32 [229376, 512], P('row', 'grp')
The draws below stay inside these ranges and needn't reach their ends.
Inputs may be any that keep to these rules, and one draw needn't show every extreme that they name: snapshots are float32 values of order one, full rank. test_block holds float32 values of order one.
All inputs are finite; a program needn't handle non-finite values.
Results may differ from the reference program's by a relative error of at most 0.0003.
Values sent between devices are 32-bit elements; how exact they have to be, the bound alone decides.
A program may use at most 64 MiB of HBM per device.

```python
import math
import jax
import jax.numpy as jnp
from jax import lax

SNAP_G = 512
RANK = 64
ITERS = 6
NROWS = 229376
SNAP = 2048
TEST = 512
WIDE = 256
N_GRP = 4


def shared_fields(key):
    base_key = jax.random.fold_in(key, 101)
    key_factor, key_scale, key_strength = jax.random.split(base_key, 3)
    factors = jnp.clip(jax.random.normal(key_factor, (NROWS, 96), jnp.float32), -4.0, 4.0)
    row_scale = jnp.exp(jax.random.uniform(key_scale, (NROWS, 1), jnp.float32, -0.5, 0.5))
    strength = jnp.exp(jax.random.uniform(key_strength, (96, 1), jnp.float32, math.log(0.3), math.log(3.0)))
    return (factors, row_scale, strength)


def build_field(key, salt, columns, weight, noise_low, noise_high):
    factors, row_scale, strength = shared_fields(key)
    own_key = jax.random.fold_in(key, salt)
    key_mix, key_noise, key_column = jax.random.split(own_key, 3)
    mixing = jnp.clip(jax.random.normal(key_mix, (96, columns), jnp.float32), -4.0, 4.0) * strength * weight
    column_scale = jnp.exp(jax.random.uniform(key_column, (1, columns), jnp.float32, math.log(noise_low), math.log(noise_high)))
    noise_part = jnp.clip(jax.random.normal(key_noise, (NROWS, columns), jnp.float32), -4.0, 4.0) * column_scale
    field = jnp.dot(factors, mixing, precision=lax.Precision.HIGHEST) + noise_part
    return jnp.clip(row_scale * field, -24.0, 24.0).astype(jnp.float32)


def draw_snapshots(key, part):
    return build_field(key, 202, SNAP, 1.0 / math.sqrt(SNAP_G), 0.3, 2.0)


def draw_test_block(key, part):
    return build_field(key, 303, TEST, 0.1, 0.3, 1.0)


def level_of(stream_key, shape, shards, low, largest):
    def one(dim, shards_of):
        steps = jax.random.uniform(jax.random.fold_in(jax.random.fold_in(stream_key, 6), dim), (shards_of,), jnp.float32, low / len(shards), largest / len(shards))
        return jnp.repeat(jnp.exp(steps), shape[dim] // shards_of).reshape((-1,) + (1,) * (len(shape) - dim - 1))

    loudness = one(*shards[0])
    for cut in shards[1:]:
        loudness = loudness * one(*cut)
    return loudness


def centred(key, extent, width, bound, cuts=(), held_as=jnp.bfloat16):
    array = jax.random.normal(key, extent, jnp.float32) * width
    if len(cuts) > 0:
        array = level_of(key, extent, cuts, -0.22, 0.18) * array
    return jnp.clip(array, min=-bound, max=bound).astype(held_as)


def setup_inputs(seed: int = 0) -> dict:
    key_list = jax.random.split(jax.random.key(seed), 5)
    snapshots = draw_snapshots(jax.random.fold_in(key_list[4], 71), 0)
    test_block = draw_test_block(jax.random.fold_in(key_list[4], 71), 0)
    start_block = centred(key_list[2], (SNAP, RANK), 1.0, 6.0, ((0, 4),), jnp.float32)
    start_merge = centred(key_list[3], (WIDE, RANK), 1.0, 6.0, (), jnp.float32)
    return dict(snapshots=snapshots, test_block=test_block, start_block=start_block, start_merge=start_merge)


def highdot(left, right):
    return jnp.dot(left.astype(jnp.float32), right.astype(jnp.float32), precision=lax.Precision.HIGHEST, preferred_element_type=jnp.float32)

def orthonormal(tall_block):
    small_gram = highdot(tall_block.T, tall_block)
    lower_factor = jnp.linalg.cholesky(small_gram)
    return lax.linalg.triangular_solve(lower_factor, tall_block, left_side=False, lower=True, transpose_a=True)

def reference(snapshots, test_block, start_block, start_merge):
    row_total = snapshots.shape[0]
    group_bases = []
    for group_index in range(N_GRP):
        columns = snapshots[:, group_index * SNAP_G:(group_index + 1) * SNAP_G]
        full_gram = highdot(columns.T, columns) / row_total
        iterate = orthonormal(start_block[group_index * SNAP_G:(group_index + 1) * SNAP_G])
        for sweep_index in range(ITERS):
            iterate = orthonormal(highdot(full_gram, iterate))
        group_bases.append(highdot(columns, iterate))
    joined = jnp.concatenate(group_bases, axis=1)
    merged_gram = highdot(joined.T, joined) / row_total
    merge_coef = orthonormal(start_merge)
    for sweep_index in range(ITERS):
        merge_coef = orthonormal(highdot(merged_gram, merge_coef))
    energy = highdot(merge_coef.T, highdot(merged_gram, merge_coef))
    lower_factor = jnp.linalg.cholesky(energy)
    merge_coef = lax.linalg.triangular_solve(lower_factor, merge_coef, left_side=False, lower=True, transpose_a=True)
    merged_modes = highdot(joined, merge_coef) / math.sqrt(row_total)
    return highdot(merged_modes, highdot(merged_modes.T, test_block))
```

```python
import functools

import jax
import jax.numpy as jnp
from jax import lax
from jax.experimental import pallas as pl
from jax.experimental.pallas import tpu as pltpu
from jax.sharding import Mesh
from jax.sharding import PartitionSpec as P

ITERS = 6
RANK = 64
ROW = ("row_0", "row_1", "row_2")
MESH = pl.DeviceIdType.MESH
F32, BF16 = jnp.float32, jnp.bfloat16
NT = (((1,), (1,)), ((), ()))
TN = (((0,), (0,)), ((), ()))
NN = (((1,), (0,)), ((), ()))
VMEM = pl.BlockSpec(memory_space=pltpu.VMEM)
GRAM_ROWS = 1536
MERGE_ROWS = 1024


def split(x):
    high = x.astype(BF16)
    return high, (x - high.astype(F32)).astype(BF16)


def bdot(a, b, dims):
    return lax.dot_general(a, b, dims, preferred_element_type=F32)


def fdot(a, b, dims=NN):
    return lax.dot_general(
        a, b, dims, precision=lax.Precision.HIGHEST, preferred_element_type=F32
    )


def lower_inverse(small):
    rows8 = lax.broadcasted_iota(jnp.int32, (8, 128), 0)
    row, lane = (lax.broadcasted_iota(jnp.int32, (64, 64), d) for d in (0, 1))
    joint = jnp.concatenate([jnp.where(row == lane, 1.0, 0.0), small], axis=1)
    bands = [joint[8 * k : 8 * k + 8, :] for k in range(8)]
    done, least, most = [], None, None
    for k in range(8):
        first = 64 + 8 * k
        cols = [
            [jnp.broadcast_to(bands[i][:, first + c : first + c + 1], (8, 128)) for c in range(8)]
            for i in range(k, 8)
        ]
        line = [jnp.broadcast_to(bands[k][a : a + 1, :], (8, 128)) for a in range(8)]
        piv = [[jnp.broadcast_to(cols[0][c][a : a + 1, :], (8, 128)) for c in range(a + 1)] for a in range(8)]
        inv, low = [None] * 8, [[None] * 8 for _ in range(8)]
        for a in range(8):
            inv[a] = 1.0 / piv[a][a]
            for c in range(a + 1, 8):
                low[c][a] = piv[c][a] * inv[a]
            for c in range(a + 1, 8):
                line[c] = line[c] - low[c][a] * line[a]
                for e in range(a + 1, c + 1):
                    piv[c][e] = piv[c][e] - low[c][a] * piv[e][a]
        band, diag = line[0], piv[0][0]
        for a in range(1, 8):
            band = jnp.where(rows8 == a, line[a], band)
            diag = jnp.where(rows8 == a, piv[a][a], diag)
        done.append(band * lax.rsqrt(diag))
        least = diag if least is None else jnp.minimum(least, diag)
        most = diag if most is None else jnp.maximum(most, diag)
        if k < 7:
            back = [line[a] * inv[a] for a in range(8)]
            for a in range(7, -1, -1):
                for c in range(a):
                    back[c] = back[c] - low[a][c] * back[a]
            for i in range(k + 1, 8):
                rest = bands[i]
                for a in range(8):
                    rest = rest - cols[i - k][a] * back[a]
                bands[i] = rest
    return jnp.concatenate(done, axis=0)[:, :64], jnp.min(least), jnp.max(most)


def orth_rows(block):
    inverse, least, most = lower_inverse(fdot(block, block, NT))
    return fdot(inverse, block), least / most


def sweeps(start, gram, out_ref, floor, last_floor):
    block, fine = start, None
    for pair in range(ITERS // 2):
        block, ratio = orth_rows(fdot(fdot(block, gram), gram))
        ok = ratio > (last_floor if pair == ITERS // 2 - 1 else floor)
        fine = ok if fine is None else jnp.logical_and(fine, ok)
    out_ref[...] = block

    @pl.when(jnp.logical_not(fine))
    def _():
        out_ref[...] = orth_rows(start)[0]

        def one(_, carry):
            out_ref[...] = orth_rows(fdot(out_ref[...], gram))[0]
            return carry

        lax.fori_loop(0, ITERS, one, 0)


def gram_kernel(x_ref, out_ref, first, second):
    step = pl.program_id(0)
    high, low = split(x_ref[...])
    one = bdot(high, high, TN)
    two = bdot(high, low, TN)

    @pl.when(step == 0)
    def _():
        first[...] = one
        second[...] = two

    @pl.when(step > 0)
    def _():
        first[...] = first[...] + one
        second[...] = second[...] + two

    @pl.when(step == pl.num_programs(0) - 1)
    def _():
        for at, (i, j) in enumerate(((0, 0), (0, 1), (1, 1))):
            block = (
                first[256 * i : 256 * i + 256, 256 * j : 256 * j + 256]
                + second[256 * i : 256 * i + 256, 256 * j : 256 * j + 256]
                + second[256 * j : 256 * j + 256, 256 * i : 256 * i + 256].T
            )
            for h in range(2):
                out_ref[512 * at + 256 * h : 512 * at + 256 * h + 256, :] = block[:, 128 * h : 128 * h + 128]


def partial_gram(snapshots):
    rows = snapshots.shape[0]
    return pl.pallas_call(
        gram_kernel,
        grid=(rows // 896,),
        in_specs=[pl.BlockSpec((896, 512), lambda i: (i, 0))],
        out_specs=pl.BlockSpec((GRAM_ROWS, 128), lambda i: (0, 0)),
        out_shape=jax.ShapeDtypeStruct((GRAM_ROWS, 128), F32),
        scratch_shapes=[pltpu.VMEM((512, 512), F32), pltpu.VMEM((512, 512), F32)],
        cost_estimate=pl.CostEstimate(flops=4 * rows * 512 * 512, bytes_accessed=rows * 2048, transcendentals=0),
        name="partial_gram",
    )(snapshots)


def sum_kernel(total, in_ref, out_ref, got1, sum1, got2, sum2, got3, send1, recv1, send2, recv2, send3, recv3):
    grp = lax.axis_index("grp")
    y, z, c = (lax.axis_index(name) for name in ROW)
    half, quarter, piece = total // 2, total // 8, total // 64
    mate = (grp, y, z, 1 - c)

    def y_peer(d):
        return lax.rem(y + d, 4)

    def z_peer(d):
        return lax.rem(z + d, 8)

    barrier = pltpu.get_barrier_semaphore()
    pl.semaphore_signal(barrier, inc=1, device_id=mate, device_id_type=MESH)
    for d in range(1, 4):
        pl.semaphore_signal(barrier, inc=1, device_id=(grp, y_peer(d), z, c), device_id_type=MESH)
    for d in range(1, 8):
        pl.semaphore_signal(barrier, inc=1, device_id=(grp, y, z_peer(d), c), device_id_type=MESH)
    pl.semaphore_wait(barrier, 11)

    def rows(start, size):
        return pl.ds(pl.multiple_of(start, 8), size)

    def copy(src, dst, send, recv, device):
        made = pltpu.make_async_remote_copy(
            src_ref=src, dst_ref=dst, send_sem=send, recv_sem=recv, device_id=device, device_id_type=MESH
        )
        made.start()
        return made

    copy(in_ref.at[rows((1 - c) * half, half)], got1, send1.at[0], recv1.at[0], mate).wait()
    sum1[...] = in_ref[rows(c * half, half), :] + got1[...]
    copies = [
        copy(sum1.at[rows(y_peer(d) * quarter, quarter)], got2.at[d - 1], send2.at[d - 1], recv2.at[d - 1],
             (grp, y_peer(d), z, c))
        for d in range(1, 4)
    ]
    for made in copies:
        made.wait()
    sum2[...] = sum1[rows(y * quarter, quarter), :] + got2[0] + got2[1] + got2[2]
    copies = [
        copy(sum2.at[rows(z_peer(d) * piece, piece)], got3.at[d - 1], send3.at[d - 1], recv3.at[d - 1],
             (grp, y, z_peer(d), c))
        for d in range(1, 8)
    ]
    for made in copies:
        made.wait()
    own = c * half + y * quarter + z * piece
    acc = sum2[rows(z * piece, piece), :]
    for d in range(7):
        acc = acc + got3[d]
    out_ref[rows(own, piece), :] = acc
    mine = out_ref.at[rows(own, piece)]
    copies = [
        copy(mine, mine, send3.at[6 + d], recv3.at[6 + d], (grp, y, z_peer(d), c)) for d in range(1, 8)
    ]
    for made in copies:
        made.wait()
    mine = out_ref.at[rows(c * half + y * quarter, quarter)]
    copies = [
        copy(mine, mine, send2.at[2 + d], recv2.at[2 + d], (grp, y_peer(d), z, c)) for d in range(1, 4)
    ]
    for made in copies:
        made.wait()
    mine = out_ref.at[rows(c * half, half)]
    copy(mine, mine, send1.at[1], recv1.at[1], mate).wait()


def sum_over_rows(array, number):
    total = array.shape[0]
    dma = pltpu.SemaphoreType.DMA
    return pl.pallas_call(
        functools.partial(sum_kernel, total),
        in_specs=[VMEM],
        out_specs=VMEM,
        out_shape=jax.ShapeDtypeStruct((total, 128), F32),
        scratch_shapes=[
            pltpu.VMEM((total // 2, 128), F32),
            pltpu.VMEM((total // 2, 128), F32),
            pltpu.VMEM((3, total // 8, 128), F32),
            pltpu.VMEM((total // 8, 128), F32),
            pltpu.VMEM((7, total // 64, 128), F32),
            dma((2,)), dma((2,)), dma((6,)), dma((6,)), dma((14,)), dma((14,)),
        ],
        compiler_params=pltpu.CompilerParams(collective_id=number, has_side_effects=True),
        name=f"sum_over_rows_{number}",
    )(array)


def basis_kernel(row_total, gram_ref, start_ref, x_ref, out_ref, gram, iterate, high_low):
    @pl.when(pl.program_id(0) == 0)
    def _():
        for at, (i, j) in enumerate(((0, 0), (0, 1), (1, 1))):
            for h in range(2):
                block = gram_ref[512 * at + 256 * h : 512 * at + 256 * h + 256, :] * (1.0 / row_total)
                gram[256 * i : 256 * i + 256, 256 * j + 128 * h : 256 * j + 128 * h + 128] = block
        gram[256:512, 0:256] = gram[0:256, 256:512].T
        sweeps(start_ref[...].T, gram[...], iterate, 1e-5, 5e-4)
        high, low = split(iterate[...])
        high_low[0:RANK, :] = high
        high_low[RANK:, :] = low

    high, low = split(x_ref[...])
    both = bdot(high_low[...], high, NT)
    out_ref[...] = both[:RANK] + both[RANK:] + bdot(high_low[0:RANK, :], low, NT)


def group_basis(gram, start_block, snapshots, row_total):
    rows = snapshots.shape[0]
    return pl.pallas_call(
        functools.partial(basis_kernel, row_total),
        grid=(rows // 512,),
        in_specs=[
            pl.BlockSpec((GRAM_ROWS, 128), lambda i: (0, 0)),
            pl.BlockSpec((512, RANK), lambda i: (0, 0)),
            pl.BlockSpec((512, 512), lambda i: (i, 0)),
        ],
        out_specs=pl.BlockSpec((RANK, 512), lambda i: (0, i)),
        out_shape=jax.ShapeDtypeStruct((RANK, rows), F32),
        scratch_shapes=[pltpu.VMEM((512, 512), F32), pltpu.VMEM((RANK, 512), F32), pltpu.VMEM((2 * RANK, 512), BF16)],
        name="group_basis",
    )(gram, start_block, snapshots)


def gather_kernel(in_ref, out_ref, send_r, recv_r, send_l, recv_l, send_f, recv_f):
    g = lax.axis_index("grp")
    y, z, c = (lax.axis_index(name) for name in ROW)
    right, left = lax.rem(g + 1, 4), lax.rem(g + 3, 4)
    part = in_ref.shape[1] // 4
    barrier = pltpu.get_barrier_semaphore()
    for peer in (right, left):
        pl.semaphore_signal(barrier, inc=1, device_id=(peer, y, z, c), device_id_type=MESH)
    pl.semaphore_wait(barrier, 2)

    def place(block, q):
        return out_ref.at[pl.ds(pl.multiple_of(block * RANK, 8), RANK), pl.ds(q * part, part)]

    def copy(src, dst, send, recv, peer):
        return pltpu.make_async_remote_copy(
            src_ref=src, dst_ref=dst, send_sem=send, recv_sem=recv, device_id=(peer, y, z, c), device_id_type=MESH
        )

    to_right = [copy(in_ref.at[:, pl.ds(q * part, part)], place(g, q), send_r.at[q], recv_r.at[q], right) for q in range(4)]
    to_left = [copy(in_ref.at[:, pl.ds(q * part, part)], place(g, q), send_l.at[q], recv_l.at[q], left) for q in range(4)]
    for q in range(4):
        to_right[q].start()
        to_left[(q + 2) % 4].start()
    out_ref[pl.ds(pl.multiple_of(g * RANK, 8), RANK), :] = in_ref[...]
    on = [copy(place(left, q), place(left, q), send_f.at[q], recv_f.at[q], right) for q in range(2)]
    on += [copy(place(right, q), place(right, q), send_f.at[q], recv_f.at[q], left) for q in (2, 3)]
    for q in range(2):
        to_right[q].wait_recv()
        on[q].start()
        to_left[q + 2].wait_recv()
        on[q + 2].start()
    for q in range(2):
        to_right[q + 2].wait_recv()
        to_left[q].wait_recv()
    for made in on:
        made.wait_recv()
    for made in to_right + to_left + on:
        made.wait_send()


def gathered(basis, number):
    rows = basis.shape[1]
    dma = pltpu.SemaphoreType.DMA
    return pl.pallas_call(
        gather_kernel,
        in_specs=[VMEM],
        out_specs=VMEM,
        out_shape=jax.ShapeDtypeStruct((4 * RANK, rows), F32),
        scratch_shapes=[dma((4,))] * 6,
        compiler_params=pltpu.CompilerParams(collective_id=number, has_side_effects=True),
        name="gathered",
    )(basis)


def merge_kernel(joined_ref, test_ref, out_ref, first, second, third):
    step = pl.program_id(0)

    @pl.when(step == 0)
    def _():
        first[...] = jnp.zeros_like(first)
        second[...] = jnp.zeros_like(second)
        third[...] = jnp.zeros_like(third)

    high, low = split(joined_ref[...])
    first[...] += bdot(high, high, NT)
    second[...] += bdot(high, low, NT)
    test_high, test_low = split(test_ref[...])
    third[...] += bdot(high, test_high, NN) + bdot(high, test_low, NN) + bdot(low, test_high, NN)

    @pl.when(step == pl.num_programs(0) - 1)
    def _():
        merged = first[...] + second[...] + second[...].T
        for h in range(2):
            out_ref[256 * h : 256 * h + 256, :] = merged[:, 128 * h : 128 * h + 128]
        out_ref[512:768, :] = third[...]
        out_ref[768:, :] = jnp.zeros((MERGE_ROWS - 768, 128), F32)


def partial_merge(joined, test_block):
    wide, rows = joined.shape
    return pl.pallas_call(
        merge_kernel,
        grid=(rows // 512,),
        in_specs=[
            pl.BlockSpec((wide, 512), lambda i: (0, i)),
            pl.BlockSpec((512, 128), lambda i: (i, 0)),
        ],
        out_specs=pl.BlockSpec((MERGE_ROWS, 128), lambda i: (0, 0)),
        out_shape=jax.ShapeDtypeStruct((MERGE_ROWS, 128), F32),
        scratch_shapes=[pltpu.VMEM((256, 256), F32), pltpu.VMEM((256, 256), F32), pltpu.VMEM((256, 128), F32)],
        name="partial_merge",
    )(joined, test_block)


def project_kernel(row_total, merge_ref, start_ref, joined_ref, out_ref, merged, iterate, factor):
    @pl.when(pl.program_id(0) == 0)
    def _():
        for h in range(2):
            merged[:, 128 * h : 128 * h + 128] = merge_ref[256 * h : 256 * h + 256, :] * (1.0 / row_total)
        sweeps(start_ref[...].T, merged[...], iterate, 3e-6, 3e-6)
        coef = iterate[...]
        energy = fdot(fdot(coef, merged[...]), coef, NT)
        coef = fdot(lower_inverse(energy)[0], coef)
        test_coeffs = fdot(coef, merge_ref[512:768, :]) * (1.0 / row_total)
        high, low = split(fdot(coef, test_coeffs, TN))
        factor[0] = high
        factor[1] = low

    high, low = split(joined_ref[...])
    out_ref[...] = bdot(high, factor[0], TN) + bdot(high, factor[1], TN) + bdot(low, factor[0], TN)


def project(merge, start_merge, joined, row_total):
    wide, rows = joined.shape
    return pl.pallas_call(
        functools.partial(project_kernel, row_total),
        grid=(rows // 512,),
        in_specs=[
            pl.BlockSpec((MERGE_ROWS, 128), lambda i: (0, 0)),
            pl.BlockSpec((256, RANK), lambda i: (0, 0)),
            pl.BlockSpec((wide, 512), lambda i: (0, i)),
        ],
        out_specs=pl.BlockSpec((512, 128), lambda i: (i, 0)),
        out_shape=jax.ShapeDtypeStruct((rows, 128), F32),
        scratch_shapes=[pltpu.VMEM((256, 256), F32), pltpu.VMEM((RANK, 256), F32), pltpu.VMEM((2, 256, 128), BF16)],
        name="project",
    )(merge, start_merge, joined)


def on_device(snapshots, test_block, start_block, start_merge):
    row_total = snapshots.shape[0] * 64
    gram = sum_over_rows(partial_gram(snapshots), 0)
    basis = group_basis(gram, start_block, snapshots, row_total)
    joined = gathered(basis, 1)
    merge = sum_over_rows(partial_merge(joined, test_block), 2)
    return project(merge, start_merge, joined, row_total)


def solution(mesh):
    finer = Mesh(
        mesh.devices.reshape(mesh.shape["grp"], 4, 8, 2), ("grp", "row_0", "row_1", "row_2")
    )
    placed = (P(ROW, "grp"), P(ROW, "grp"), P("grp", None), P())
    return jax.shard_map(
        on_device, mesh=finer, in_specs=placed, out_specs=P(ROW, "grp"), check_vma=False
    )
```

```python
import functools

import jax
import jax.numpy as jnp
from jax import lax
from jax.experimental import pallas as pl
from jax.experimental.pallas import tpu as pltpu
from jax.sharding import Mesh
from jax.sharding import PartitionSpec as P

ITERS = 6
RANK = 64
ROW = ("row_0", "row_1", "row_2")
MESH = pl.DeviceIdType.MESH
F32, BF16 = jnp.float32, jnp.bfloat16
NT = (((1,), (1,)), ((), ()))
TN = (((0,), (0,)), ((), ()))
NN = (((1,), (0,)), ((), ()))
VMEM = pl.BlockSpec(memory_space=pltpu.VMEM)
GRAM_ROWS = 1536
MERGE_ROWS = 1024


def split(x):
    high = x.astype(BF16)
    return high, (x - high.astype(F32)).astype(BF16)


def bdot(a, b, dims):
    return lax.dot_general(a, b, dims, preferred_element_type=F32)


def fdot(a, b, dims=NN):
    return lax.dot_general(
        a, b, dims, precision=lax.Precision.HIGHEST, preferred_element_type=F32
    )


def lower_inverse(small):
    rows8 = lax.broadcasted_iota(jnp.int32, (8, 128), 0)
    row, lane = (lax.broadcasted_iota(jnp.int32, (64, 64), d) for d in (0, 1))
    joint = jnp.concatenate([jnp.where(row == lane, 1.0, 0.0), small], axis=1)
    bands = [joint[8 * k : 8 * k + 8, :] for k in range(8)]
    done, least, most = [], None, None
    for k in range(8):
        first = 64 + 8 * k
        cols = [
            [jnp.broadcast_to(bands[i][:, first + c : first + c + 1], (8, 128)) for c in range(8)]
            for i in range(k, 8)
        ]
        line = [jnp.broadcast_to(bands[k][a : a + 1, :], (8, 128)) for a in range(8)]
        piv = [[jnp.broadcast_to(cols[0][c][a : a + 1, :], (8, 128)) for c in range(a + 1)] for a in range(8)]
        inv, low = [None] * 8, [[None] * 8 for _ in range(8)]
        for a in range(8):
            inv[a] = 1.0 / piv[a][a]
            for c in range(a + 1, 8):
                low[c][a] = piv[c][a] * inv[a]
            for c in range(a + 1, 8):
                line[c] = line[c] - low[c][a] * line[a]
                for e in range(a + 1, c + 1):
                    piv[c][e] = piv[c][e] - low[c][a] * piv[e][a]
        band, diag = line[0], piv[0][0]
        for a in range(1, 8):
            band = jnp.where(rows8 == a, line[a], band)
            diag = jnp.where(rows8 == a, piv[a][a], diag)
        done.append(band * lax.rsqrt(diag))
        least = diag if least is None else jnp.minimum(least, diag)
        most = diag if most is None else jnp.maximum(most, diag)
        if k < 7:
            back = [line[a] * inv[a] for a in range(8)]
            for a in range(7, -1, -1):
                for c in range(a):
                    back[c] = back[c] - low[a][c] * back[a]
            for i in range(k + 1, 8):
                rest = bands[i]
                for a in range(8):
                    rest = rest - cols[i - k][a] * back[a]
                bands[i] = rest
    return jnp.concatenate(done, axis=0)[:, :64], jnp.min(least), jnp.max(most)


def split3(x):
    high = x.astype(BF16)
    rest = x - high.astype(F32)
    mid = rest.astype(BF16)
    return high, mid, (rest - mid.astype(F32)).astype(BF16)


def times(block, parts):
    three = jnp.concatenate(split3(block), axis=0)
    n = block.shape[0]
    one = bdot(three, parts[0], NN)
    two = bdot(three[: 2 * n], parts[1], NN)
    return one[:n] + ((one[n : 2 * n] + two[:n]) + (one[2 * n :] + two[n:]))


def orth_rows(block):
    inverse, least, most = lower_inverse(fdot(block, block, NT))
    return fdot(inverse, block), least / most


def sweeps(start, parts, out_ref, floor, last_floor):
    block, fine = start, None
    for pair in range(ITERS // 2):
        block, ratio = orth_rows(times(times(block, parts), parts))
        ok = ratio > (last_floor if pair == ITERS // 2 - 1 else floor)
        fine = ok if fine is None else jnp.logical_and(fine, ok)
    out_ref[...] = block

    @pl.when(jnp.logical_not(fine))
    def _():
        out_ref[...] = orth_rows(start)[0]

        def one(_, carry):
            out_ref[...] = orth_rows(times(out_ref[...], parts))[0]
            return carry

        lax.fori_loop(0, ITERS, one, 0)


def gram_kernel(x_ref, out_ref, first, second):
    step = pl.program_id(0)
    high, low = split(x_ref[...])
    one = bdot(high, high, TN)
    two = bdot(high, low, TN)

    @pl.when(step == 0)
    def _():
        first[...] = one
        second[...] = two

    @pl.when(step > 0)
    def _():
        first[...] = first[...] + one
        second[...] = second[...] + two

    @pl.when(step == pl.num_programs(0) - 1)
    def _():
        for at, (i, j) in enumerate(((0, 0), (0, 1), (1, 1))):
            block = (
                first[256 * i : 256 * i + 256, 256 * j : 256 * j + 256]
                + second[256 * i : 256 * i + 256, 256 * j : 256 * j + 256]
                + second[256 * j : 256 * j + 256, 256 * i : 256 * i + 256].T
            )
            for h in range(2):
                out_ref[512 * at + 256 * h : 512 * at + 256 * h + 256, :] = block[:, 128 * h : 128 * h + 128]


def partial_gram(snapshots):
    rows = snapshots.shape[0]
    return pl.pallas_call(
        gram_kernel,
        grid=(rows // 896,),
        in_specs=[pl.BlockSpec((896, 512), lambda i: (i, 0))],
        out_specs=pl.BlockSpec((GRAM_ROWS, 128), lambda i: (0, 0)),
        out_shape=jax.ShapeDtypeStruct((GRAM_ROWS, 128), F32),
        scratch_shapes=[pltpu.VMEM((512, 512), F32), pltpu.VMEM((512, 512), F32)],
        cost_estimate=pl.CostEstimate(flops=4 * rows * 512 * 512, bytes_accessed=rows * 2048, transcendentals=0),
        name="partial_gram",
    )(snapshots)


def rows_at(start, size):
    return pl.ds(pl.multiple_of(start, 8), size)


def remote(src, dst, send, recv, device):
    return pltpu.make_async_remote_copy(
        src_ref=src, dst_ref=dst, send_sem=send, recv_sem=recv, device_id=device, device_id_type=MESH
    )


def row_peers():
    grp = lax.axis_index("grp")
    y, z, c = (lax.axis_index(name) for name in ROW)
    along_y = [(lax.rem(y + d, 4), (grp, lax.rem(y + d, 4), z, c)) for d in range(1, 4)]
    along_z = [(lax.rem(z + d, 8), (grp, y, lax.rem(z + d, 8), c)) for d in range(1, 8)]
    return (grp, y, z, 1 - c), along_y, along_z


def greet(peers):
    barrier = pltpu.get_barrier_semaphore()
    for peer in peers:
        pl.semaphore_signal(barrier, inc=1, device_id=peer, device_id_type=MESH)
    pl.semaphore_wait(barrier, len(peers))


class StagedSum:
    def __init__(self, in_ref, out_ref, got1, sum1, got2, sum2, got3, send, recv):
        self.in_ref, self.out_ref = in_ref, out_ref
        self.got1, self.sum1, self.got2, self.sum2, self.got3 = got1, sum1, got2, sum2, got3
        self.send, self.recv = send, recv
        self.mate, self.along_y, self.along_z = row_peers()
        self.y, self.z, self.c = (lax.axis_index(name) for name in ROW)

    def copy(self, i, at, src, dst, device):
        return remote(src, dst, self.send.at[i, at], self.recv.at[i, at], device)

    def halves(self, i):
        src = self.in_ref.at[rows_at(512 * i + (1 - self.c) * 256, 256)]
        return [self.copy(i, 0, src, self.got1.at[i], self.mate)]

    def quarters(self, i):
        return [
            self.copy(i, 1 + d, self.sum1.at[i, rows_at(y * 64, 64)], self.got2.at[i, d], peer)
            for d, (y, peer) in enumerate(self.along_y)
        ]

    def eighths(self, i):
        return [
            self.copy(i, 4 + d, self.sum2.at[i, rows_at(z * 8, 8)], self.got3.at[i, d], peer)
            for d, (z, peer) in enumerate(self.along_z)
        ]

    def back_z(self, i):
        mine = self.out_ref.at[rows_at(512 * i + self.c * 256 + self.y * 64 + self.z * 8, 8)]
        return [self.copy(i, 11 + d, mine, mine, peer) for d, (_, peer) in enumerate(self.along_z)]

    def back_y(self, i):
        mine = self.out_ref.at[rows_at(512 * i + self.c * 256 + self.y * 64, 64)]
        return [self.copy(i, 18 + d, mine, mine, peer) for d, (_, peer) in enumerate(self.along_y)]

    def back_core(self, i):
        mine = self.out_ref.at[rows_at(512 * i + self.c * 256, 256)]
        return [self.copy(i, 21, mine, mine, self.mate)]

    def add(self, stage, i):
        if stage == 0:
            self.sum1[i] = self.in_ref[rows_at(512 * i + self.c * 256, 256), :] + self.got1[i]
        elif stage == 1:
            self.sum2[i] = self.sum1[i, rows_at(self.y * 64, 64), :] + self.got2[i, 0] + self.got2[i, 1] + self.got2[i, 2]
        elif stage == 2:
            total = self.sum2[i, rows_at(self.z * 8, 8), :]
            for d in range(7):
                total = total + self.got3[i, d]
            self.out_ref[rows_at(512 * i + self.c * 256 + self.y * 64 + self.z * 8, 8), :] = total

    def start(self, made):
        for one in made:
            one.start()
        return made

    def finish(self, flying):
        stages = [self.halves, self.quarters, self.eighths, self.back_z, self.back_y, self.back_core]
        for stage in range(6):
            for i in range(len(flying)):
                for one in flying[i]:
                    one.wait()
                self.add(stage, i)
                if stage < 5:
                    flying[i] = self.start(stages[stage + 1](i))


def sum_scratch(chunks):
    dma = pltpu.SemaphoreType.DMA
    return [
        pltpu.VMEM((chunks, 256, 128), F32),
        pltpu.VMEM((chunks, 256, 128), F32),
        pltpu.VMEM((chunks, 3, 64, 128), F32),
        pltpu.VMEM((chunks, 64, 128), F32),
        pltpu.VMEM((chunks, 7, 8, 128), F32),
        dma((chunks, 22)),
        dma((chunks, 22)),
    ]


def sum_kernel(in_ref, out_ref, *scratch):
    work = StagedSum(in_ref, out_ref, *scratch)
    greet([work.mate] + [peer for _, peer in work.along_y + work.along_z])
    work.finish([work.start(work.halves(i)) for i in range(in_ref.shape[0] // 512)])


def sum_over_rows(array, number):
    total = array.shape[0]
    return pl.pallas_call(
        sum_kernel,
        in_specs=[VMEM],
        out_specs=VMEM,
        out_shape=jax.ShapeDtypeStruct((total, 128), F32),
        scratch_shapes=sum_scratch(total // 512),
        compiler_params=pltpu.CompilerParams(collective_id=number, has_side_effects=True),
        name="sum_over_rows",
    )(array)


def basis_kernel(row_total, gram_ref, start_ref, x_ref, out_ref, gram, iterate, high_low):
    @pl.when(pl.program_id(0) == 0)
    def _():
        for at, (i, j) in enumerate(((0, 0), (0, 1), (1, 1))):
            for h in range(2):
                block = gram_ref[512 * at + 256 * h : 512 * at + 256 * h + 256, :] * (1.0 / row_total)
                gram[256 * i : 256 * i + 256, 256 * j + 128 * h : 256 * j + 128 * h + 128] = block
        gram[256:512, 0:256] = gram[0:256, 256:512].T
        sweeps(start_ref[...], split(gram[...]), iterate, 1e-5, 5e-4)
        high, low = split(iterate[...])
        high_low[0:RANK, :] = high
        high_low[RANK:, :] = low

    high, low = split(x_ref[...])
    both = bdot(high_low[...], high, NT)
    out_ref[...] = both[:RANK] + both[RANK:] + bdot(high_low[0:RANK, :], low, NT)


def group_basis(gram, start_block, snapshots, row_total):
    rows = snapshots.shape[0]
    return pl.pallas_call(
        functools.partial(basis_kernel, row_total),
        grid=(rows // 512,),
        in_specs=[
            pl.BlockSpec((GRAM_ROWS, 128), lambda i: (0, 0)),
            pl.BlockSpec((RANK, 512), lambda i: (0, 0)),
            pl.BlockSpec((512, 512), lambda i: (i, 0)),
        ],
        out_specs=pl.BlockSpec((RANK, 512), lambda i: (0, i)),
        out_shape=jax.ShapeDtypeStruct((RANK, rows), F32),
        scratch_shapes=[pltpu.VMEM((512, 512), F32), pltpu.VMEM((RANK, 512), F32), pltpu.VMEM((2 * RANK, 512), BF16)],
        name="group_basis",
    )(gram, start_block, snapshots)


def merge_products(q, joined_ref, test_ref, first, second, third):
    part = test_ref.shape[0] // 4
    high, low = split(joined_ref[:, q * part : (q + 1) * part])
    test_high, test_low = split(test_ref[q * part : (q + 1) * part, :])
    one = bdot(high, high, NT)
    two = bdot(high, low, NT)
    three = bdot(high, test_high, NN) + bdot(high, test_low, NN) + bdot(low, test_high, NN)
    if q == 0:
        first[...], second[...], third[...] = one, two, three
    else:
        first[...] = first[...] + one
        second[...] = second[...] + two
        third[...] = third[...] + three


def merge_kernel(in_ref, test_ref, out_ref, merge_ref, part_ref, first, second, third, send_g, recv_g, *scratch):
    g = lax.axis_index("grp")
    y, z, c = (lax.axis_index(name) for name in ROW)
    right, left = lax.rem(g + 1, 4), lax.rem(g + 3, 4)
    part = in_ref.shape[1] // 4
    work = StagedSum(part_ref, merge_ref, *scratch)
    greet([(right, y, z, c), (left, y, z, c), work.mate] + [peer for _, peer in work.along_y + work.along_z])

    def place(block, q, first_row, size):
        return out_ref.at[rows_at(block * RANK + first_row, size), pl.ds(q * part, part)]

    def own(q):
        src = in_ref.at[:, pl.ds(q * part, part)]
        return [
            remote(src, place(g, q, 0, RANK), send_g.at[k, q], recv_g.at[k, q], (peer, y, z, c))
            for k, peer in enumerate((right, left))
        ]

    def on(q):
        return [
            remote(place(block, q, at, 32), place(block, q, at, 32), send_g.at[k, q], recv_g.at[k, q], (peer, y, z, c))
            for k, block, at, peer in ((2, left, 0, right), (3, right, 32, left))
        ]

    owns, ons = [own(q) for q in range(4)], [on(q) for q in range(4)]

    def start(made):
        for one in made:
            one.start()

    def arrived(made):
        for one in made:
            one.wait_recv()

    start(owns[0])
    start(owns[1])
    out_ref[rows_at(g * RANK, RANK), :] = in_ref[...]
    for q in range(4):
        arrived(owns[q])
        start(ons[q])
        if q < 2:
            start(owns[q + 2])
        if q > 0:
            arrived(ons[q - 1])
            merge_products(q - 1, out_ref, test_ref, first, second, third)
    arrived(ons[3])
    merge_products(3, out_ref, test_ref, first, second, third)
    merged = first[...] + second[...] + second[...].T
    for h in range(2):
        part_ref[256 * h : 256 * h + 256, :] = merged[:, 128 * h : 128 * h + 128]
    part_ref[512:768, :] = third[...]
    part_ref[768:, :] = jnp.zeros((MERGE_ROWS - 768, 128), F32)
    work.finish([work.start(work.halves(i)) for i in range(MERGE_ROWS // 512)])
    for made in owns + ons:
        for one in made:
            one.wait_send()


def merged_over_rows(basis, test_block, number):
    rows = basis.shape[1]
    dma = pltpu.SemaphoreType.DMA
    return pl.pallas_call(
        merge_kernel,
        in_specs=[VMEM, VMEM],
        out_specs=[VMEM, VMEM],
        out_shape=[jax.ShapeDtypeStruct((4 * RANK, rows), F32), jax.ShapeDtypeStruct((MERGE_ROWS, 128), F32)],
        scratch_shapes=[
            pltpu.VMEM((MERGE_ROWS, 128), F32),
            pltpu.VMEM((256, 256), F32),
            pltpu.VMEM((256, 256), F32),
            pltpu.VMEM((256, 128), F32),
            dma((4, 4)),
            dma((4, 4)),
        ] + sum_scratch(MERGE_ROWS // 512),
        compiler_params=pltpu.CompilerParams(
            collective_id=number, has_side_effects=True, vmem_limit_bytes=48 * 1024 * 1024
        ),
        name="merged_over_rows",
    )(basis, test_block)


def project_kernel(row_total, merge_ref, start_ref, joined_ref, out_ref, merged, iterate, factor):
    @pl.when(pl.program_id(0) == 0)
    def _():
        for h in range(2):
            merged[:, 128 * h : 128 * h + 128] = merge_ref[256 * h : 256 * h + 256, :] * (1.0 / row_total)
        parts = split(merged[...])
        sweeps(start_ref[...], parts, iterate, 3e-6, 3e-6)
        coef = iterate[...]
        energy = fdot(times(coef, parts), coef, NT)
        coef = fdot(lower_inverse(energy)[0], coef)
        test_coeffs = fdot(coef, merge_ref[512:768, :]) * (1.0 / row_total)
        high, low = split(fdot(coef, test_coeffs, TN))
        factor[0] = high
        factor[1] = low

    high, low = split(joined_ref[...])
    out_ref[...] = bdot(high, factor[0], TN) + bdot(high, factor[1], TN) + bdot(low, factor[0], TN)


def project(merge, start_merge, joined, row_total):
    wide, rows = joined.shape
    return pl.pallas_call(
        functools.partial(project_kernel, row_total),
        grid=(rows // 512,),
        in_specs=[
            pl.BlockSpec((MERGE_ROWS, 128), lambda i: (0, 0)),
            pl.BlockSpec((RANK, 256), lambda i: (0, 0)),
            pl.BlockSpec((wide, 512), lambda i: (0, i)),
        ],
        out_specs=pl.BlockSpec((512, 128), lambda i: (i, 0)),
        out_shape=jax.ShapeDtypeStruct((rows, 128), F32),
        scratch_shapes=[pltpu.VMEM((256, 256), F32), pltpu.VMEM((RANK, 256), F32), pltpu.VMEM((2, 256, 128), BF16)],
        name="project",
    )(merge, start_merge, joined)


def on_device(snapshots, test_block, start_block, start_merge):
    row_total = snapshots.shape[0] * 64
    gram = sum_over_rows(partial_gram(snapshots), 0)
    basis = group_basis(gram, start_block.T, snapshots, row_total)
    joined, merge = merged_over_rows(basis, test_block, 1)
    return project(merge, start_merge.T, joined, row_total)


def solution(mesh):
    finer = Mesh(
        mesh.devices.reshape(mesh.shape["grp"], 4, 8, 2), ("grp", "row_0", "row_1", "row_2")
    )
    placed = (P(ROW, "grp"), P(ROW, "grp"), P("grp", None), P())
    return jax.shard_map(
        on_device, mesh=finer, in_specs=placed, out_specs=P(ROW, "grp"), check_vma=False
    )
```

```python
import functools

import jax
import jax.numpy as jnp
from jax import lax
from jax.experimental import pallas as pl
from jax.experimental.pallas import tpu as pltpu
from jax.sharding import Mesh
from jax.sharding import PartitionSpec as P

ITERS = 6
RANK = 64
ROW = ("row_0", "row_1", "row_2")
MESH = pl.DeviceIdType.MESH
F32, BF16 = jnp.float32, jnp.bfloat16
NT = (((1,), (1,)), ((), ()))
TN = (((0,), (0,)), ((), ()))
NN = (((1,), (0,)), ((), ()))
VMEM = pl.BlockSpec(memory_space=pltpu.VMEM)
GRAM_ROWS = 1536
MERGE_ROWS = 1024


def split(x):
    high = x.astype(BF16)
    return high, (x - high.astype(F32)).astype(BF16)


def bdot(a, b, dims):
    return lax.dot_general(a, b, dims, preferred_element_type=F32)


def fdot(a, b, dims=NN):
    return lax.dot_general(
        a, b, dims, precision=lax.Precision.HIGHEST, preferred_element_type=F32
    )


def lower_inverse(small):
    rows8 = lax.broadcasted_iota(jnp.int32, (8, 128), 0)
    row, lane = (lax.broadcasted_iota(jnp.int32, (64, 64), d) for d in (0, 1))
    joint = jnp.concatenate([jnp.where(row == lane, 1.0, 0.0), small], axis=1)
    bands = [joint[8 * k : 8 * k + 8, :] for k in range(8)]
    done, least, most = [], None, None
    for k in range(8):
        first = 64 + 8 * k
        cols = [
            [jnp.broadcast_to(bands[i][:, first + c : first + c + 1], (8, 128)) for c in range(8)]
            for i in range(k, 8)
        ]
        line = [jnp.broadcast_to(bands[k][a : a + 1, :], (8, 128)) for a in range(8)]
        piv = [[jnp.broadcast_to(cols[0][c][a : a + 1, :], (8, 128)) for c in range(a + 1)] for a in range(8)]
        inv, low = [None] * 8, [[None] * 8 for _ in range(8)]
        for a in range(8):
            inv[a] = 1.0 / piv[a][a]
            for c in range(a + 1, 8):
                low[c][a] = piv[c][a] * inv[a]
            for c in range(a + 1, 8):
                line[c] = line[c] - low[c][a] * line[a]
                for e in range(a + 1, c + 1):
                    piv[c][e] = piv[c][e] - low[c][a] * piv[e][a]
        band, diag = line[0], piv[0][0]
        for a in range(1, 8):
            band = jnp.where(rows8 == a, line[a], band)
            diag = jnp.where(rows8 == a, piv[a][a], diag)
        done.append(band * lax.rsqrt(diag))
        least = diag if least is None else jnp.minimum(least, diag)
        most = diag if most is None else jnp.maximum(most, diag)
        if k < 7:
            back = [line[a] * inv[a] for a in range(8)]
            for a in range(7, -1, -1):
                for c in range(a):
                    back[c] = back[c] - low[a][c] * back[a]
            for i in range(k + 1, 8):
                rest = bands[i]
                for a in range(8):
                    rest = rest - cols[i - k][a] * back[a]
                bands[i] = rest
    return jnp.concatenate(done, axis=0)[:, :64], jnp.min(least), jnp.max(most)


def split3(x):
    high = x.astype(BF16)
    rest = x - high.astype(F32)
    mid = rest.astype(BF16)
    return high, mid, (rest - mid.astype(F32)).astype(BF16)


def times(block, parts):
    three = jnp.concatenate(split3(block), axis=0)
    n = block.shape[0]
    one = bdot(three, parts[0], NN)
    two = bdot(three[: 2 * n], parts[1], NN)
    return one[:n] + ((one[n : 2 * n] + two[:n]) + (one[2 * n :] + two[n:]))


def orth_rows(block):
    inverse, least, most = lower_inverse(fdot(block, block, NT))
    return fdot(inverse, block), least / most


def corrected(block, images):
    row, lane = (lax.broadcasted_iota(jnp.int32, (RANK, RANK), d) for d in (0, 1))
    excess = fdot(block, images, NT) - jnp.where(row == lane, 1.0, 0.0)
    part = jnp.where(row > lane, excess, jnp.where(row == lane, 0.5 * excess, 0.0))
    return block - fdot(part, block), jnp.sum(excess * excess)


def step_by_step(start, parts, out_ref):
    out_ref[...] = orth_rows(start)[0]

    def one(_, carry):
        out_ref[...] = orth_rows(times(out_ref[...], parts))[0]
        return carry

    lax.fori_loop(0, ITERS, one, 0)


def rows_at(start, size):
    return pl.ds(pl.multiple_of(start, 8), size)


def remote(src, dst, send, recv, device):
    return pltpu.make_async_remote_copy(
        src_ref=src, dst_ref=dst, send_sem=send, recv_sem=recv, device_id=device, device_id_type=MESH
    )


def row_peers():
    grp = lax.axis_index("grp")
    y, z, c = (lax.axis_index(name) for name in ROW)
    along_y = [(lax.rem(y + d, 4), (grp, lax.rem(y + d, 4), z, c)) for d in range(1, 4)]
    along_z = [(lax.rem(z + d, 8), (grp, y, lax.rem(z + d, 8), c)) for d in range(1, 8)]
    return (grp, y, z, 1 - c), along_y, along_z


def greet(peers):
    barrier = pltpu.get_barrier_semaphore()
    for peer in peers:
        pl.semaphore_signal(barrier, inc=1, device_id=peer, device_id_type=MESH)


def meet(peers):
    pl.semaphore_wait(pltpu.get_barrier_semaphore(), len(peers))


def pieces_in(src, dst, sem):
    part = src.shape[0] // 4
    made = [
        pltpu.make_async_copy(src.at[pl.ds(q * part, part)], dst.at[pl.ds(q * part, part)], sem.at[q]) for q in range(4)
    ]
    for one in made:
        one.start()
    return made


class StagedSum:
    def __init__(self, in_ref, out_ref, got1, sum1, got2, sum2, got3, send, recv):
        self.in_ref, self.out_ref = in_ref, out_ref
        self.got1, self.sum1, self.got2, self.sum2, self.got3 = got1, sum1, got2, sum2, got3
        self.send, self.recv = send, recv
        self.stage, self.flying = {}, {}
        self.mate, self.along_y, self.along_z = row_peers()
        self.y, self.z, self.c = (lax.axis_index(name) for name in ROW)

    def copy(self, i, at, src, dst, device):
        return remote(src, dst, self.send.at[i, at], self.recv.at[i, at], device)

    def halves(self, i):
        src = self.in_ref.at[rows_at(512 * i + (1 - self.c) * 256, 256)]
        return [self.copy(i, 0, src, self.got1.at[i], self.mate)]

    def quarters(self, i):
        return [
            self.copy(i, 1 + d, self.sum1.at[i, rows_at(y * 64, 64)], self.got2.at[i, d], peer)
            for d, (y, peer) in enumerate(self.along_y)
        ]

    def eighths(self, i):
        return [
            self.copy(i, 4 + d, self.sum2.at[i, rows_at(z * 8, 8)], self.got3.at[i, d], peer)
            for d, (z, peer) in enumerate(self.along_z)
        ]

    def back_z(self, i):
        mine = self.out_ref.at[rows_at(512 * i + self.c * 256 + self.y * 64 + self.z * 8, 8)]
        return [self.copy(i, 11 + d, mine, mine, peer) for d, (_, peer) in enumerate(self.along_z)]

    def back_y(self, i):
        mine = self.out_ref.at[rows_at(512 * i + self.c * 256 + self.y * 64, 64)]
        return [self.copy(i, 18 + d, mine, mine, peer) for d, (_, peer) in enumerate(self.along_y)]

    def back_core(self, i):
        mine = self.out_ref.at[rows_at(512 * i + self.c * 256, 256)]
        return [self.copy(i, 21, mine, mine, self.mate)]

    def add(self, stage, i):
        if stage == 0:
            self.sum1[i] = self.in_ref[rows_at(512 * i + self.c * 256, 256), :] + self.got1[i]
        elif stage == 1:
            self.sum2[i] = self.sum1[i, rows_at(self.y * 64, 64), :] + self.got2[i, 0] + self.got2[i, 1] + self.got2[i, 2]
        elif stage == 2:
            total = self.sum2[i, rows_at(self.z * 8, 8), :]
            for d in range(7):
                total = total + self.got3[i, d]
            self.out_ref[rows_at(512 * i + self.c * 256 + self.y * 64 + self.z * 8, 8), :] = total

    def begin(self, i):
        self.stage[i], self.flying[i] = 0, self.halves(i)
        for one in self.flying[i]:
            one.start()

    def advance(self, i):
        for one in self.flying[i]:
            one.wait()
        stage = self.stage[i]
        self.add(stage, i)
        self.stage[i] = stage + 1
        if stage < 5:
            following = (self.quarters, self.eighths, self.back_z, self.back_y, self.back_core)[stage]
            self.flying[i] = following(i)
            for one in self.flying[i]:
                one.start()

    def finish(self):
        while min(self.stage.values()) < 6:
            low = min(self.stage.values())
            for i in sorted(self.stage):
                if self.stage[i] == low:
                    self.advance(i)


def sum_scratch(chunks):
    dma = pltpu.SemaphoreType.DMA
    return [
        pltpu.VMEM((chunks, 256, 128), F32),
        pltpu.VMEM((chunks, 256, 128), F32),
        pltpu.VMEM((chunks, 3, 64, 128), F32),
        pltpu.VMEM((chunks, 64, 128), F32),
        pltpu.VMEM((chunks, 7, 8, 128), F32),
        dma((chunks, 22)),
        dma((chunks, 22)),
    ]


def pack(at, block, out_ref):
    for h in range(2):
        out_ref[512 * at + 256 * h : 512 * at + 256 * h + 256, :] = block[:, 128 * h : 128 * h + 128]


def gram_first(x_pieces, x_ref, high_ref, low_ref, out_ref):
    part = x_ref.shape[0] // 4
    one = two = None
    for q in range(4):
        x_pieces[q].wait()
        here = slice(q * part, q * part + part)
        high, low = split(x_ref[here, :])
        high_ref[here, :], low_ref[here, :] = high, low
        a, b = bdot(high[:, :256], high[:, :256], TN), bdot(high[:, :256], low[:, :256], TN)
        one, two = (a, b) if one is None else (one + a, two + b)
    pack(0, one + two + two.T, out_ref)


def gram_second(high_ref, low_ref, out_ref):
    left, right = high_ref[:, :256], high_ref[:, 256:]
    pack(1, bdot(left, right, TN) + bdot(left, low_ref[:, 256:], TN) + bdot(low_ref[:, :256], right, TN), out_ref)


def gram_third(high_ref, low_ref, out_ref):
    both = bdot(high_ref[:, 256:], jnp.concatenate([high_ref[:, 256:], low_ref[:, 256:]], axis=1), TN)
    pack(2, both[:, :256] + both[:, 256:] + both[:, 256:].T, out_ref)


def gram_kernel(x_hbm, out_ref, x_ref, high_ref, low_ref, part_ref, x_sem, *scratch):
    work = StagedSum(part_ref, out_ref, *scratch)
    peers = [work.mate] + [peer for _, peer in work.along_y + work.along_z]
    x_pieces = pieces_in(x_hbm, x_ref, x_sem)
    greet(peers)
    gram_first(x_pieces, x_ref, high_ref, low_ref, part_ref)
    meet(peers)
    work.begin(0)
    gram_second(high_ref, low_ref, part_ref)
    work.begin(1)
    work.advance(0)
    gram_third(high_ref, low_ref, part_ref)
    work.begin(2)
    work.advance(1)
    work.advance(0)
    work.finish()


def gram_over_rows(snapshots, number):
    rows = snapshots.shape[0]
    return pl.pallas_call(
        gram_kernel,
        in_specs=[pl.BlockSpec(memory_space=pl.ANY)],
        out_specs=VMEM,
        out_shape=jax.ShapeDtypeStruct((GRAM_ROWS, 128), F32),
        scratch_shapes=[
            pltpu.VMEM((rows, 512), F32),
            pltpu.VMEM((rows, 512), BF16),
            pltpu.VMEM((rows, 512), BF16),
            pltpu.VMEM((GRAM_ROWS, 128), F32),
            pltpu.SemaphoreType.DMA((4,)),
        ] + sum_scratch(GRAM_ROWS // 512),
        compiler_params=pltpu.CompilerParams(
            collective_id=number, has_side_effects=True, vmem_limit_bytes=48 * 1024 * 1024
        ),
        name="gram_over_rows",
    )(snapshots)


def solve_kernel(row_total, gram_ref, start_ref, out_ref, gram):
    for at, (i, j) in enumerate(((0, 0), (0, 1), (1, 1))):
        for h in range(2):
            block = gram_ref[512 * at + 256 * h : 512 * at + 256 * h + 256, :] * (1.0 / row_total)
            gram[256 * i : 256 * i + 256, 256 * j + 128 * h : 256 * j + 128 * h + 128] = block
    gram[256:512, 0:256] = gram[0:256, 256:512].T
    parts = split(gram[...])
    block, ratio = orth_rows(times(times(times(start_ref[...], parts), parts), parts))
    block, last_ratio = orth_rows(times(times(times(block, parts), parts), parts))
    block, error = corrected(block, block)
    out_ref[...] = block
    fine = jnp.logical_and(jnp.minimum(ratio, last_ratio) > 3e-6, error < 1e-5)

    @pl.when(jnp.logical_not(fine))
    def _():
        step_by_step(start_ref[...], parts, out_ref)


def group_solve(gram, start_block, row_total):
    return pl.pallas_call(
        functools.partial(solve_kernel, row_total),
        in_specs=[VMEM, VMEM],
        out_specs=VMEM,
        out_shape=jax.ShapeDtypeStruct((RANK, 512), F32),
        scratch_shapes=[pltpu.VMEM((512, 512), F32)],
        name="group_solve",
    )(gram, start_block)


def merge_products(q, joined_ref, test_ref, first, second, third):
    part = test_ref.shape[0] // 4
    high, low = split(joined_ref[:, q * part : (q + 1) * part])
    test_high, test_low = split(test_ref[q * part : (q + 1) * part, :])
    one = bdot(high, high, NT)
    two = bdot(high, low, NT)
    three = bdot(high, test_high, NN) + bdot(high, test_low, NN) + bdot(low, test_high, NN)
    if q == 0:
        first[...], second[...], third[...] = one, two, three
    else:
        first[...] = first[...] + one
        second[...] = second[...] + two
        third[...] = third[...] + three


def basis_piece(high_low, x):
    high, low = split(x)
    both = bdot(high_low, high, NT)
    return both[:RANK] + both[RANK:] + bdot(high_low[:RANK], low, NT)


def merge_kernel(
    iterate_ref, x_hbm, test_ref, out_ref, merge_ref, x_ref, part_ref, first, second, third, x_sem, send_g, recv_g, *scratch
):
    g = lax.axis_index("grp")
    y, z, c = (lax.axis_index(name) for name in ROW)
    right, left = lax.rem(g + 1, 4), lax.rem(g + 3, 4)
    part = x_ref.shape[0] // 4
    x_pieces = pieces_in(x_hbm, x_ref, x_sem)
    work = StagedSum(part_ref, merge_ref, *scratch)
    peers = [(right, y, z, c), (left, y, z, c), work.mate] + [peer for _, peer in work.along_y + work.along_z]
    greet(peers)
    high_low = jnp.concatenate(split(iterate_ref[...]), axis=0)

    def place(block, q, first_row, size):
        return out_ref.at[rows_at(block * RANK + first_row, size), pl.ds(q * part, part)]

    def own(q):
        return [
            remote(place(g, q, 0, RANK), place(g, q, 0, RANK), send_g.at[k, q], recv_g.at[k, q], (peer, y, z, c))
            for k, peer in enumerate((right, left))
        ]

    def on(q):
        return [
            remote(place(block, q, at, 32), place(block, q, at, 32), send_g.at[k, q], recv_g.at[k, q], (peer, y, z, c))
            for k, block, at, peer in ((2, left, 0, right), (3, right, 32, left))
        ]

    owns, ons = [own(q) for q in range(4)], [on(q) for q in range(4)]

    def start(made):
        for one in made:
            one.start()

    def arrived(made):
        for one in made:
            one.wait_recv()

    def make(q):
        x_pieces[q].wait()
        out_ref[rows_at(g * RANK, RANK), q * part : (q + 1) * part] = basis_piece(
            high_low, x_ref[q * part : (q + 1) * part, :]
        )

    make(0)
    meet(peers)
    start(owns[0])
    make(1)
    start(owns[1])
    make(2)
    for q in range(4):
        arrived(owns[q])
        start(ons[q])
        if q < 2:
            start(owns[q + 2])
        if q == 0:
            make(3)
        else:
            arrived(ons[q - 1])
            merge_products(q - 1, out_ref, test_ref, first, second, third)
    arrived(ons[3])
    merge_products(3, out_ref, test_ref, first, second, third)
    merged = first[...] + second[...] + second[...].T
    for h in range(2):
        part_ref[256 * h : 256 * h + 256, :] = merged[:, 128 * h : 128 * h + 128]
    work.begin(0)
    part_ref[512:768, :] = third[...]
    part_ref[768:, :] = jnp.zeros((MERGE_ROWS - 768, 128), F32)
    work.begin(1)
    work.finish()
    for made in owns + ons:
        for one in made:
            one.wait_send()


def merged_over_rows(iterate, snapshots, test_block, number):
    rows = snapshots.shape[0]
    dma = pltpu.SemaphoreType.DMA
    return pl.pallas_call(
        merge_kernel,
        in_specs=[VMEM, pl.BlockSpec(memory_space=pl.ANY), VMEM],
        out_specs=[VMEM, VMEM],
        out_shape=[jax.ShapeDtypeStruct((4 * RANK, rows), F32), jax.ShapeDtypeStruct((MERGE_ROWS, 128), F32)],
        scratch_shapes=[
            pltpu.VMEM((rows, 512), F32),
            pltpu.VMEM((MERGE_ROWS, 128), F32),
            pltpu.VMEM((256, 256), F32),
            pltpu.VMEM((256, 256), F32),
            pltpu.VMEM((256, 128), F32),
            dma((4,)),
            dma((4, 4)),
            dma((4, 4)),
        ] + sum_scratch(MERGE_ROWS // 512),
        compiler_params=pltpu.CompilerParams(
            collective_id=number, has_side_effects=True, vmem_limit_bytes=48 * 1024 * 1024
        ),
        name="merged_over_rows",
    )(iterate, snapshots, test_block)


def project_kernel(row_total, merge_ref, start_ref, joined_ref, out_ref, merged, coef_ref, factor):
    @pl.when(pl.program_id(0) == 0)
    def _():
        for h in range(2):
            merged[:, 128 * h : 128 * h + 128] = merge_ref[256 * h : 256 * h + 256, :] * (1.0 / row_total)
        parts = split(merged[...])

        def to_modes(block):
            inverse, _, _ = lower_inverse(fdot(times(block, parts), block, NT))
            block = fdot(inverse, block)
            return corrected(block, times(block, parts))

        block, ratio = orth_rows(times(times(start_ref[...], parts), parts))
        block, next_ratio = orth_rows(times(times(block, parts), parts))
        coef, error = to_modes(times(times(block, parts), parts))
        coef_ref[...] = coef
        fine = jnp.logical_and(jnp.minimum(ratio, next_ratio) > 3e-6, error < 1e-4)

        @pl.when(jnp.logical_not(fine))
        def _():
            step_by_step(start_ref[...], parts, coef_ref)
            coef_ref[...] = to_modes(coef_ref[...])[0]

        coef = coef_ref[...]
        test_coeffs = fdot(coef, merge_ref[512:768, :]) * (1.0 / row_total)
        high, low = split(fdot(test_coeffs, coef, TN))
        factor[0:128, :] = high
        factor[128:, :] = low

    high, low = split(joined_ref[...])
    both = bdot(factor[...], high, NN)
    out_ref[...] = (both[:128] + both[128:] + bdot(factor[0:128, :], low, NN)).T


def project(merge, start_merge, joined, row_total):
    wide, rows = joined.shape
    return pl.pallas_call(
        functools.partial(project_kernel, row_total),
        grid=(rows // 512,),
        in_specs=[
            pl.BlockSpec((MERGE_ROWS, 128), lambda i: (0, 0)),
            pl.BlockSpec((RANK, 256), lambda i: (0, 0)),
            pl.BlockSpec((wide, 512), lambda i: (0, i)),
        ],
        out_specs=pl.BlockSpec((512, 128), lambda i: (i, 0)),
        out_shape=jax.ShapeDtypeStruct((rows, 128), F32),
        scratch_shapes=[pltpu.VMEM((256, 256), F32), pltpu.VMEM((RANK, 256), F32), pltpu.VMEM((256, 256), BF16)],
        name="project",
    )(merge, start_merge, joined)


def on_device(snapshots, test_block, start_block, start_merge):
    row_total = snapshots.shape[0] * 64
    gram = gram_over_rows(snapshots, 0)
    iterate = group_solve(gram, start_block.T, row_total)
    joined, merge = merged_over_rows(iterate, snapshots, test_block, 1)
    return project(merge, start_merge.T, joined, row_total)


def solution(mesh):
    finer = Mesh(
        mesh.devices.reshape(mesh.shape["grp"], 4, 8, 2), ("grp", "row_0", "row_1", "row_2")
    )
    placed = (P(ROW, "grp"), P(ROW, "grp"), P("grp", None), P())
    return jax.shard_map(
        on_device, mesh=finer, in_specs=placed, out_specs=P(ROW, "grp"), check_vma=False
    )
```

```python
import functools

import jax
import jax.numpy as jnp
from jax import lax
from jax.experimental import pallas as pl
from jax.experimental.pallas import tpu as pltpu
from jax.sharding import Mesh
from jax.sharding import PartitionSpec as P

ITERS = 6
RANK = 64
ROW = ("row_0", "row_1", "row_2")
MESH = pl.DeviceIdType.MESH
F32, BF16 = jnp.float32, jnp.bfloat16
NT = (((1,), (1,)), ((), ()))
TN = (((0,), (0,)), ((), ()))
NN = (((1,), (0,)), ((), ()))
VMEM = pl.BlockSpec(memory_space=pltpu.VMEM)
GRAM_ROWS = 1536
MERGE_ROWS = 1024


def split(x):
    high = x.astype(BF16)
    return high, (x - high.astype(F32)).astype(BF16)


def bdot(a, b, dims):
    return lax.dot_general(a, b, dims, preferred_element_type=F32)


def fdot(a, b, dims=NN):
    return lax.dot_general(
        a, b, dims, precision=lax.Precision.HIGHEST, preferred_element_type=F32
    )


def spread(x):
    return jnp.broadcast_to(x, (8, 128))


def lower_inverse(small):
    rows8 = lax.broadcasted_iota(jnp.int32, (8, 128), 0)
    row, lane = (lax.broadcasted_iota(jnp.int32, (64, 64), d) for d in (0, 1))
    joint = jnp.concatenate([jnp.where(row == lane, 1.0, 0.0), small], axis=1)
    bands = [joint[8 * k : 8 * k + 8, :] for k in range(8)]
    done, least, most = [], None, None
    for k in range(8):
        first = 64 + 8 * k
        cols = [[spread(bands[i][:, first + c : first + c + 1]) for c in range(8)] for i in range(k, 8)]
        line = [spread(bands[k][a : a + 1, :]) for a in range(8)]
        piv = [[spread(cols[0][c][a : a + 1, :]) for c in range(a + 1)] for a in range(8)]
        for a in range(8):
            inv = 1.0 / piv[a][a]
            low = {c: piv[c][a] * inv for c in range(a + 1, 8)}
            for c in range(a + 1, 8):
                for e in range(a + 1, c + 1):
                    piv[c][e] = piv[c][e] - low[c] * piv[e][a]
            for c in range(a + 1, 8):
                line[c] = line[c] - low[c] * line[a]
            for i in range(1, 8 - k):
                share = cols[i][a] * inv
                bands[k + i] = bands[k + i] - share * line[a]
                for c in range(a + 1, 8):
                    cols[i][c] = cols[i][c] - share * piv[c][a]
        band, diag = line[0], piv[0][0]
        for a in range(1, 8):
            band = jnp.where(rows8 == a, line[a], band)
            diag = jnp.where(rows8 == a, piv[a][a], diag)
        done.append(band * lax.rsqrt(diag))
        least = diag if least is None else jnp.minimum(least, diag)
        most = diag if most is None else jnp.maximum(most, diag)
    return jnp.concatenate(done, axis=0)[:, :64], jnp.min(least), jnp.max(most)


def split3(x):
    high = x.astype(BF16)
    rest = x - high.astype(F32)
    mid = rest.astype(BF16)
    return high, mid, (rest - mid.astype(F32)).astype(BF16)


def times(block, parts):
    three = jnp.concatenate(split3(block), axis=0)
    n = block.shape[0]
    one = bdot(three, parts[0], NN)
    two = bdot(three[: 2 * n], parts[1], NN)
    low = one[2 * n :] + two[n:] + bdot(three[:n], parts[2], NN)
    return one[:n] + ((one[n : 2 * n] + two[:n]) + low)


def orth_rows(block):
    inverse, least, most = lower_inverse(fdot(block, block, NT))
    return fdot(inverse, block), least / most


def corrected(block, images):
    row, lane = (lax.broadcasted_iota(jnp.int32, (RANK, RANK), d) for d in (0, 1))
    excess = fdot(block, images, NT) - jnp.where(row == lane, 1.0, 0.0)
    part = jnp.where(row > lane, excess, jnp.where(row == lane, 0.5 * excess, 0.0))
    return block - fdot(part, block), jnp.sum(excess * excess)


def step_by_step(start, parts, out_ref):
    out_ref[...] = orth_rows(start)[0]

    def one(_, carry):
        out_ref[...] = orth_rows(times(out_ref[...], parts))[0]
        return carry

    lax.fori_loop(0, ITERS, one, 0)


def rows_at(start, size):
    return pl.ds(pl.multiple_of(start, 8), size)


def remote(src, dst, send, recv, device):
    return pltpu.make_async_remote_copy(
        src_ref=src, dst_ref=dst, send_sem=send, recv_sem=recv, device_id=device, device_id_type=MESH
    )


def row_peers():
    grp = lax.axis_index("grp")
    y, z, c = (lax.axis_index(name) for name in ROW)
    along_y = [(lax.rem(y + d, 4), (grp, lax.rem(y + d, 4), z, c)) for d in range(1, 4)]
    along_z = [(lax.rem(z + d, 8), (grp, y, lax.rem(z + d, 8), c)) for d in range(1, 8)]
    return (grp, y, z, 1 - c), along_y, along_z


def greet(peers):
    barrier = pltpu.get_barrier_semaphore()
    for peer in peers:
        pl.semaphore_signal(barrier, inc=1, device_id=peer, device_id_type=MESH)


def meet(peers):
    pl.semaphore_wait(pltpu.get_barrier_semaphore(), len(peers))


def pieces_in(src, dst, sem):
    count = sem.shape[0]
    part = src.shape[0] // count
    made = [
        pltpu.make_async_copy(src.at[pl.ds(q * part, part)], dst.at[pl.ds(q * part, part)], sem.at[q])
        for q in range(count)
    ]
    for one in made:
        one.start()
    return made


class StagedSum:
    def __init__(self, in_ref, out_ref, got1, sum1, got2, sum2, got3, send, recv):
        self.in_ref, self.out_ref = in_ref, out_ref
        self.got1, self.sum1, self.got2, self.sum2, self.got3 = got1, sum1, got2, sum2, got3
        self.send, self.recv = send, recv
        self.stage, self.flying = {}, {}
        self.mate, self.along_y, self.along_z = row_peers()
        self.y, self.z, self.c = (lax.axis_index(name) for name in ROW)

    def copy(self, i, at, src, dst, device):
        return remote(src, dst, self.send.at[i, at], self.recv.at[i, at], device)

    def halves(self, i):
        src = self.in_ref.at[rows_at(512 * i + (1 - self.c) * 256, 256)]
        return [self.copy(i, 0, src, self.got1.at[i], self.mate)]

    def quarters(self, i):
        return [
            self.copy(i, 1 + d, self.sum1.at[i, rows_at(y * 64, 64)], self.got2.at[i, d], peer)
            for d, (y, peer) in enumerate(self.along_y)
        ]

    def eighths(self, i):
        return [
            self.copy(i, 4 + d, self.sum2.at[i, rows_at(z * 8, 8)], self.got3.at[i, d], peer)
            for d, (z, peer) in enumerate(self.along_z)
        ]

    def back_z(self, i):
        mine = self.out_ref.at[rows_at(512 * i + self.c * 256 + self.y * 64 + self.z * 8, 8)]
        return [self.copy(i, 11 + d, mine, mine, peer) for d, (_, peer) in enumerate(self.along_z)]

    def back_y(self, i):
        mine = self.out_ref.at[rows_at(512 * i + self.c * 256 + self.y * 64, 64)]
        return [self.copy(i, 18 + d, mine, mine, peer) for d, (_, peer) in enumerate(self.along_y)]

    def back_core(self, i):
        mine = self.out_ref.at[rows_at(512 * i + self.c * 256, 256)]
        return [self.copy(i, 21, mine, mine, self.mate)]

    def add(self, stage, i):
        if stage == 0:
            self.sum1[i] = self.in_ref[rows_at(512 * i + self.c * 256, 256), :] + self.got1[i]
        elif stage == 1:
            self.sum2[i] = self.sum1[i, rows_at(self.y * 64, 64), :] + self.got2[i, 0] + self.got2[i, 1] + self.got2[i, 2]
        elif stage == 2:
            total = self.sum2[i, rows_at(self.z * 8, 8), :]
            for d in range(7):
                total = total + self.got3[i, d]
            self.out_ref[rows_at(512 * i + self.c * 256 + self.y * 64 + self.z * 8, 8), :] = total

    def begin(self, i):
        self.stage[i], self.flying[i] = 0, self.halves(i)
        for one in self.flying[i]:
            one.start()

    def advance(self, i):
        for one in self.flying[i]:
            one.wait()
        stage = self.stage[i]
        self.add(stage, i)
        self.stage[i] = stage + 1
        if stage < 5:
            following = (self.quarters, self.eighths, self.back_z, self.back_y, self.back_core)[stage]
            self.flying[i] = following(i)
            for one in self.flying[i]:
                one.start()

    def finish(self):
        while min(self.stage.values()) < 6:
            low = min(self.stage.values())
            for i in sorted(self.stage):
                if self.stage[i] == low:
                    self.advance(i)


def sum_scratch(chunks):
    dma = pltpu.SemaphoreType.DMA
    return [
        pltpu.VMEM((chunks, 256, 128), F32),
        pltpu.VMEM((chunks, 256, 128), F32),
        pltpu.VMEM((chunks, 3, 64, 128), F32),
        pltpu.VMEM((chunks, 64, 128), F32),
        pltpu.VMEM((chunks, 7, 8, 128), F32),
        dma((chunks, 22)),
        dma((chunks, 22)),
    ]


def pack(at, block, out_ref):
    for h in range(2):
        out_ref[512 * at + 256 * h : 512 * at + 256 * h + 256, :] = block[:, 128 * h : 128 * h + 128]


def gram_first(x_pieces, x_ref, high_ref, low_ref, out_ref):
    part = x_ref.shape[0] // 4
    one = two = None
    for q in range(4):
        x_pieces[q].wait()
        here = slice(q * part, q * part + part)
        high, low = split(x_ref[here, :])
        high_ref[here, :], low_ref[here, :] = high, low
        a, b = bdot(high[:, :256], high[:, :256], TN), bdot(high[:, :256], low[:, :256], TN)
        one, two = (a, b) if one is None else (one + a, two + b)
    pack(0, one + two + two.T, out_ref)


def gram_second(high_ref, low_ref, out_ref):
    left, right = high_ref[:, :256], high_ref[:, 256:]
    pack(1, bdot(left, right, TN) + bdot(left, low_ref[:, 256:], TN) + bdot(low_ref[:, :256], right, TN), out_ref)


def gram_third(high_ref, low_ref, out_ref):
    both = bdot(high_ref[:, 256:], jnp.concatenate([high_ref[:, 256:], low_ref[:, 256:]], axis=1), TN)
    pack(2, both[:, :256] + both[:, 256:] + both[:, 256:].T, out_ref)


def gram_kernel(x_hbm, out_ref, x_ref, high_ref, low_ref, part_ref, x_sem, *scratch):
    work = StagedSum(part_ref, out_ref, *scratch)
    peers = [work.mate] + [peer for _, peer in work.along_y + work.along_z]
    x_pieces = pieces_in(x_hbm, x_ref, x_sem)
    greet(peers)
    gram_first(x_pieces, x_ref, high_ref, low_ref, part_ref)
    meet(peers)
    work.begin(0)
    gram_second(high_ref, low_ref, part_ref)
    work.begin(1)
    work.advance(0)
    gram_third(high_ref, low_ref, part_ref)
    work.begin(2)
    work.advance(1)
    work.advance(0)
    work.finish()


def gram_over_rows(snapshots, number):
    rows = snapshots.shape[0]
    return pl.pallas_call(
        gram_kernel,
        in_specs=[pl.BlockSpec(memory_space=pl.ANY)],
        out_specs=VMEM,
        out_shape=jax.ShapeDtypeStruct((GRAM_ROWS, 128), F32),
        scratch_shapes=[
            pltpu.VMEM((rows, 512), F32),
            pltpu.VMEM((rows, 512), BF16),
            pltpu.VMEM((rows, 512), BF16),
            pltpu.VMEM((GRAM_ROWS, 128), F32),
            pltpu.SemaphoreType.DMA((4,)),
        ] + sum_scratch(GRAM_ROWS // 512),
        compiler_params=pltpu.CompilerParams(
            collective_id=number, has_side_effects=True, vmem_limit_bytes=48 * 1024 * 1024
        ),
        name="gram_over_rows",
    )(snapshots)


def solve_kernel(row_total, gram_ref, start_ref, out_ref, gram):
    for at, (i, j) in enumerate(((0, 0), (0, 1), (1, 1))):
        for h in range(2):
            block = gram_ref[512 * at + 256 * h : 512 * at + 256 * h + 256, :] * (1.0 / row_total)
            gram[256 * i : 256 * i + 256, 256 * j + 128 * h : 256 * j + 128 * h + 128] = block
    gram[256:512, 0:256] = gram[0:256, 256:512].T
    parts = split3(gram[...])
    block, ratio = orth_rows(times(times(times(start_ref[...], parts), parts), parts))
    block, last_ratio = orth_rows(times(times(times(block, parts), parts), parts))
    block, error = corrected(block, block)
    out_ref[...] = block
    fine = jnp.logical_and(jnp.minimum(ratio, last_ratio) > 3e-6, error < 1e-5)

    @pl.when(jnp.logical_not(fine))
    def _():
        step_by_step(start_ref[...], parts, out_ref)


def group_solve(gram, start_block, row_total):
    return pl.pallas_call(
        functools.partial(solve_kernel, row_total),
        in_specs=[VMEM, VMEM],
        out_specs=VMEM,
        out_shape=jax.ShapeDtypeStruct((RANK, 512), F32),
        scratch_shapes=[pltpu.VMEM((512, 512), F32)],
        compiler_params=pltpu.CompilerParams(vmem_limit_bytes=16 * 1024 * 1024),
        name="group_solve",
    )(gram, start_block)


PIECES = 7


def merge_products(q, joined_ref, test_ref, first, second, third):
    part = test_ref.shape[0] // PIECES
    high, low = split(joined_ref[:, q * part : (q + 1) * part])
    test_high, test_low = split(test_ref[q * part : (q + 1) * part, :])
    one = bdot(high, high, NT)
    two = bdot(high, low, NT)
    three = bdot(high, test_high, NN) + bdot(high, test_low, NN) + bdot(low, test_high, NN)
    if q == 0:
        first[...], second[...], third[...] = one, two, three
    else:
        first[...] = first[...] + one
        second[...] = second[...] + two
        third[...] = third[...] + three


def basis_piece(high_low, x):
    high, low = split(x)
    both = bdot(high_low, high, NT)
    return both[:RANK] + both[RANK:] + bdot(high_low[:RANK], low, NT)


def merge_kernel(
    iterate_ref, x_hbm, test_ref, out_ref, merge_ref, x_ref, part_ref, first, second, third, x_sem, send_g, recv_g, *scratch
):
    g = lax.axis_index("grp")
    y, z, c = (lax.axis_index(name) for name in ROW)
    right, left = lax.rem(g + 1, 4), lax.rem(g + 3, 4)
    part = x_ref.shape[0] // PIECES
    x_pieces = pieces_in(x_hbm, x_ref, x_sem)
    work = StagedSum(part_ref, merge_ref, *scratch)
    peers = [(right, y, z, c), (left, y, z, c), work.mate] + [peer for _, peer in work.along_y + work.along_z]
    greet(peers)
    high_low = jnp.concatenate(split(iterate_ref[...]), axis=0)

    def place(block, q, first_row, size):
        return out_ref.at[rows_at(block * RANK + first_row, size), pl.ds(q * part, part)]

    def own(q):
        return [
            remote(place(g, q, 0, RANK), place(g, q, 0, RANK), send_g.at[k, q], recv_g.at[k, q], (peer, y, z, c))
            for k, peer in enumerate((right, left))
        ]

    def on(q):
        return [
            remote(place(block, q, at, 32), place(block, q, at, 32), send_g.at[k, q], recv_g.at[k, q], (peer, y, z, c))
            for k, block, at, peer in ((2, left, 0, right), (3, right, 32, left))
        ]

    owns, ons = [own(q) for q in range(PIECES)], [on(q) for q in range(PIECES)]

    def start(made):
        for one in made:
            one.start()

    def arrived(made):
        for one in made:
            one.wait_recv()

    def make(q):
        x_pieces[q].wait()
        out_ref[rows_at(g * RANK, RANK), q * part : (q + 1) * part] = basis_piece(
            high_low, x_ref[q * part : (q + 1) * part, :]
        )

    make(0)
    meet(peers)
    start(owns[0])
    make(1)
    start(owns[1])
    make(2)
    for q in range(PIECES):
        arrived(owns[q])
        start(ons[q])
        if q + 2 < PIECES:
            start(owns[q + 2])
        if q + 3 < PIECES:
            make(q + 3)
        if q > 0:
            arrived(ons[q - 1])
            merge_products(q - 1, out_ref, test_ref, first, second, third)
    arrived(ons[PIECES - 1])
    merge_products(PIECES - 1, out_ref, test_ref, first, second, third)
    merged = first[...] + second[...] + second[...].T
    for h in range(2):
        part_ref[256 * h : 256 * h + 256, :] = merged[:, 128 * h : 128 * h + 128]
    work.begin(0)
    part_ref[512:768, :] = third[...]
    part_ref[768:, :] = jnp.zeros((MERGE_ROWS - 768, 128), F32)
    work.begin(1)
    work.finish()
    for made in owns + ons:
        for one in made:
            one.wait_send()


def merged_over_rows(iterate, snapshots, test_block, number):
    rows = snapshots.shape[0]
    dma = pltpu.SemaphoreType.DMA
    return pl.pallas_call(
        merge_kernel,
        in_specs=[VMEM, pl.BlockSpec(memory_space=pl.ANY), VMEM],
        out_specs=[VMEM, VMEM],
        out_shape=[jax.ShapeDtypeStruct((4 * RANK, rows), F32), jax.ShapeDtypeStruct((MERGE_ROWS, 128), F32)],
        scratch_shapes=[
            pltpu.VMEM((rows, 512), F32),
            pltpu.VMEM((MERGE_ROWS, 128), F32),
            pltpu.VMEM((256, 256), F32),
            pltpu.VMEM((256, 256), F32),
            pltpu.VMEM((256, 128), F32),
            dma((PIECES,)),
            dma((4, PIECES)),
            dma((4, PIECES)),
        ] + sum_scratch(MERGE_ROWS // 512),
        compiler_params=pltpu.CompilerParams(
            collective_id=number, has_side_effects=True, vmem_limit_bytes=48 * 1024 * 1024
        ),
        name="merged_over_rows",
    )(iterate, snapshots, test_block)


def project_kernel(row_total, merge_ref, start_ref, joined_ref, out_ref, merged, coef_ref, factor):
    @pl.when(pl.program_id(0) == 0)
    def _():
        for h in range(2):
            merged[:, 128 * h : 128 * h + 128] = merge_ref[256 * h : 256 * h + 256, :] * (1.0 / row_total)
        parts = split3(merged[...])

        def to_modes(block):
            inverse, _, _ = lower_inverse(fdot(times(block, parts), block, NT))
            block = fdot(inverse, block)
            return corrected(block, times(block, parts))

        block, ratio = orth_rows(times(times(start_ref[...], parts), parts))
        block, next_ratio = orth_rows(times(times(block, parts), parts))
        coef, error = to_modes(times(times(block, parts), parts))
        coef_ref[...] = coef
        fine = jnp.logical_and(jnp.minimum(ratio, next_ratio) > 3e-6, error < 1e-4)

        @pl.when(jnp.logical_not(fine))
        def _():
            step_by_step(start_ref[...], parts, coef_ref)
            coef_ref[...] = to_modes(coef_ref[...])[0]

        coef = coef_ref[...]
        test_coeffs = fdot(coef, merge_ref[512:768, :]) * (1.0 / row_total)
        high, low = split(fdot(test_coeffs, coef, TN))
        factor[0:128, :] = high
        factor[128:, :] = low

    size = out_ref.shape[0]
    here = pl.ds(pl.multiple_of(pl.program_id(0) * size, 128), size)
    high, low = split(joined_ref[:, here])
    both = bdot(factor[...], high, NN)
    out_ref[...] = (both[:128] + both[128:] + bdot(factor[0:128, :], low, NN)).T


def project(merge, start_merge, joined, row_total):
    rows = joined.shape[1]
    return pl.pallas_call(
        functools.partial(project_kernel, row_total),
        grid=(rows // 512,),
        in_specs=[VMEM, VMEM, VMEM],
        out_specs=pl.BlockSpec((512, 128), lambda i: (i, 0)),
        out_shape=jax.ShapeDtypeStruct((rows, 128), F32),
        scratch_shapes=[pltpu.VMEM((256, 256), F32), pltpu.VMEM((RANK, 256), F32), pltpu.VMEM((256, 256), BF16)],
        compiler_params=pltpu.CompilerParams(vmem_limit_bytes=16 * 1024 * 1024),
        name="project",
    )(merge, start_merge, joined)


def on_device(snapshots, test_block, start_block, start_merge):
    row_total = snapshots.shape[0] * 64
    gram = gram_over_rows(snapshots, 0)
    iterate = group_solve(gram, start_block.T, row_total)
    joined, merge = merged_over_rows(iterate, snapshots, test_block, 1)
    return project(merge, start_merge.T, joined, row_total)


def solution(mesh):
    finer = Mesh(
        mesh.devices.reshape(mesh.shape["grp"], 4, 8, 2), ("grp", "row_0", "row_1", "row_2")
    )
    placed = (P(ROW, "grp"), P(ROW, "grp"), P("grp", None), P())
    return jax.shard_map(
        on_device, mesh=finer, in_specs=placed, out_specs=P(ROW, "grp"), check_vma=False
    )
```

```python
import functools

import jax
import jax.numpy as jnp
from jax import lax
from jax.experimental import pallas as pl
from jax.experimental.pallas import tpu as pltpu
from jax.sharding import Mesh
from jax.sharding import PartitionSpec as P

ITERS = 6
RANK = 64
ROW = ("row_0", "row_1", "row_2")
MESH = pl.DeviceIdType.MESH
F32, BF16 = jnp.float32, jnp.bfloat16
NT = (((1,), (1,)), ((), ()))
TN = (((0,), (0,)), ((), ()))
NN = (((1,), (0,)), ((), ()))
VMEM = pl.BlockSpec(memory_space=pltpu.VMEM)
GRAM_ROWS = 1536
MERGE_ROWS = 1024


def split(x):
    high = x.astype(BF16)
    return high, (x - high.astype(F32)).astype(BF16)


def bdot(a, b, dims):
    return lax.dot_general(a, b, dims, preferred_element_type=F32)


def fdot(a, b, dims=NN):
    return lax.dot_general(
        a, b, dims, precision=lax.Precision.HIGHEST, preferred_element_type=F32
    )


def spread(x):
    return jnp.broadcast_to(x, (8, 128))


def lower_inverse(small):
    rows8 = lax.broadcasted_iota(jnp.int32, (8, 128), 0)
    row, lane = (lax.broadcasted_iota(jnp.int32, (64, 64), d) for d in (0, 1))
    joint = jnp.concatenate([jnp.where(row == lane, 1.0, 0.0), small], axis=1)
    bands = [joint[8 * k : 8 * k + 8, :] for k in range(8)]
    done, least, most = [], None, None
    corner = [spread(bands[0][:, 64 + c : 65 + c]) for c in range(8)]
    for k in range(8):
        first = 64 + 8 * k
        cols = [corner]
        cols += [[spread(bands[i][:, first + c : first + c + 1]) for c in range(8)] for i in range(k + 1, 8)]
        if k < 7:
            corner = [spread(bands[k + 1][:, first + 8 + c : first + 9 + c]) for c in range(8)]
        line = [spread(bands[k][a : a + 1, :]) for a in range(8)]
        piv = [[spread(cols[0][c][a : a + 1, :]) for c in range(a + 1)] for a in range(8)]
        for a in range(8):
            inv = 1.0 / piv[a][a]
            low = {c: piv[c][a] * inv for c in range(a + 1, 8)}
            for c in range(a + 1, 8):
                for e in range(a + 1, c + 1):
                    piv[c][e] = piv[c][e] - low[c] * piv[e][a]
            for c in range(a + 1, 8):
                line[c] = line[c] - low[c] * line[a]
            for i in range(1, 8 - k):
                share = cols[i][a] * inv
                bands[k + i] = bands[k + i] - share * line[a]
                if i == 1:
                    corner = [corner[c] - share * spread(cols[1][a][c : c + 1, :]) for c in range(8)]
                for c in range(a + 1, 8):
                    cols[i][c] = cols[i][c] - share * piv[c][a]
        band, diag = line[0], piv[0][0]
        for a in range(1, 8):
            band = jnp.where(rows8 == a, line[a], band)
            diag = jnp.where(rows8 == a, piv[a][a], diag)
        done.append(band * lax.rsqrt(diag))
        least = diag if least is None else jnp.minimum(least, diag)
        most = diag if most is None else jnp.maximum(most, diag)
    return jnp.concatenate(done, axis=0)[:, :64], jnp.min(least), jnp.max(most)


def split3(x):
    high = x.astype(BF16)
    rest = x - high.astype(F32)
    mid = rest.astype(BF16)
    return high, mid, (rest - mid.astype(F32)).astype(BF16)


def times(block, parts):
    three = jnp.concatenate(split3(block), axis=0)
    n = block.shape[0]
    one = bdot(three, parts[0], NN)
    two = bdot(three[: 2 * n], parts[1], NN)
    low = one[2 * n :] + two[n:] + bdot(three[:n], parts[2], NN)
    return one[:n] + ((one[n : 2 * n] + two[:n]) + low)


def orth_rows(block):
    inverse, least, most = lower_inverse(fdot(block, block, NT))
    return fdot(inverse, block), least / most


def corrected(block, images):
    row, lane = (lax.broadcasted_iota(jnp.int32, (RANK, RANK), d) for d in (0, 1))
    excess = fdot(block, images, NT) - jnp.where(row == lane, 1.0, 0.0)
    part = jnp.where(row > lane, excess, jnp.where(row == lane, 0.5 * excess, 0.0))
    return block - fdot(part, block), jnp.sum(excess * excess)


def step_by_step(start, parts, out_ref):
    out_ref[...] = orth_rows(start)[0]

    def one(_, carry):
        out_ref[...] = orth_rows(times(out_ref[...], parts))[0]
        return carry

    lax.fori_loop(0, ITERS, one, 0)


def rows_at(start, size):
    return pl.ds(pl.multiple_of(start, 8), size)


def remote(src, dst, send, recv, device):
    return pltpu.make_async_remote_copy(
        src_ref=src, dst_ref=dst, send_sem=send, recv_sem=recv, device_id=device, device_id_type=MESH
    )


def row_peers():
    grp = lax.axis_index("grp")
    y, z, c = (lax.axis_index(name) for name in ROW)
    along_y = [(lax.rem(y + d, 4), (grp, lax.rem(y + d, 4), z, c)) for d in range(1, 4)]
    along_z = [(lax.rem(z + d, 8), (grp, y, lax.rem(z + d, 8), c)) for d in range(1, 8)]
    return (grp, y, z, 1 - c), along_y, along_z


def greet(peers):
    barrier = pltpu.get_barrier_semaphore()
    for peer in peers:
        pl.semaphore_signal(barrier, inc=1, device_id=peer, device_id_type=MESH)


def meet(peers):
    pl.semaphore_wait(pltpu.get_barrier_semaphore(), len(peers))


def pieces_in(src, dst, sem):
    count = sem.shape[0]
    part = src.shape[0] // count
    made = [
        pltpu.make_async_copy(src.at[pl.ds(q * part, part)], dst.at[pl.ds(q * part, part)], sem.at[q])
        for q in range(count)
    ]
    for one in made:
        one.start()
    return made


class StagedSum:
    def __init__(self, in_ref, out_ref, got1, sum1, got2, sum2, got3, send, recv):
        self.in_ref, self.out_ref = in_ref, out_ref
        self.got1, self.sum1, self.got2, self.sum2, self.got3 = got1, sum1, got2, sum2, got3
        self.send, self.recv = send, recv
        self.stage, self.flying = {}, {}
        self.mate, self.along_y, self.along_z = row_peers()
        self.y, self.z, self.c = (lax.axis_index(name) for name in ROW)

    def copy(self, i, at, src, dst, device):
        return remote(src, dst, self.send.at[i, at], self.recv.at[i, at], device)

    def halves(self, i):
        src = self.in_ref.at[rows_at(512 * i + (1 - self.c) * 256, 256)]
        return [self.copy(i, 0, src, self.got1.at[i], self.mate)]

    def quarters(self, i):
        return [
            self.copy(i, 1 + d, self.sum1.at[i, rows_at(y * 64, 64)], self.got2.at[i, d], peer)
            for d, (y, peer) in enumerate(self.along_y)
        ]

    def eighths(self, i):
        return [
            self.copy(i, 4 + d, self.sum2.at[i, rows_at(z * 8, 8)], self.got3.at[i, d], peer)
            for d, (z, peer) in enumerate(self.along_z)
        ]

    def back_z(self, i):
        mine = self.out_ref.at[rows_at(512 * i + self.c * 256 + self.y * 64 + self.z * 8, 8)]
        return [self.copy(i, 11 + d, mine, mine, peer) for d, (_, peer) in enumerate(self.along_z)]

    def back_y(self, i):
        mine = self.out_ref.at[rows_at(512 * i + self.c * 256 + self.y * 64, 64)]
        return [self.copy(i, 18 + d, mine, mine, peer) for d, (_, peer) in enumerate(self.along_y)]

    def back_core(self, i):
        mine = self.out_ref.at[rows_at(512 * i + self.c * 256, 256)]
        return [self.copy(i, 21, mine, mine, self.mate)]

    def add(self, stage, i):
        if stage == 0:
            self.sum1[i] = self.in_ref[rows_at(512 * i + self.c * 256, 256), :] + self.got1[i]
        elif stage == 1:
            self.sum2[i] = self.sum1[i, rows_at(self.y * 64, 64), :] + self.got2[i, 0] + self.got2[i, 1] + self.got2[i, 2]
        elif stage == 2:
            total = self.sum2[i, rows_at(self.z * 8, 8), :]
            for d in range(7):
                total = total + self.got3[i, d]
            self.out_ref[rows_at(512 * i + self.c * 256 + self.y * 64 + self.z * 8, 8), :] = total

    def begin(self, i):
        self.stage[i], self.flying[i] = 0, self.halves(i)
        for one in self.flying[i]:
            one.start()

    def advance(self, i):
        for one in self.flying[i]:
            one.wait()
        stage = self.stage[i]
        self.add(stage, i)
        self.stage[i] = stage + 1
        if stage < 5:
            following = (self.quarters, self.eighths, self.back_z, self.back_y, self.back_core)[stage]
            self.flying[i] = following(i)
            for one in self.flying[i]:
                one.start()

    def finish(self):
        while min(self.stage.values()) < 6:
            low = min(self.stage.values())
            for i in sorted(self.stage):
                if self.stage[i] == low:
                    self.advance(i)


def sum_scratch(chunks):
    dma = pltpu.SemaphoreType.DMA
    return [
        pltpu.VMEM((chunks, 256, 128), F32),
        pltpu.VMEM((chunks, 256, 128), F32),
        pltpu.VMEM((chunks, 3, 64, 128), F32),
        pltpu.VMEM((chunks, 64, 128), F32),
        pltpu.VMEM((chunks, 7, 8, 128), F32),
        dma((chunks, 22)),
        dma((chunks, 22)),
    ]


def pack(at, block, out_ref):
    for h in range(2):
        out_ref[512 * at + 256 * h : 512 * at + 256 * h + 256, :] = block[:, 128 * h : 128 * h + 128]


def gram_first(x_pieces, x_ref, high_ref, low_ref, out_ref):
    part = x_ref.shape[0] // 4
    one = two = None
    for q in range(4):
        x_pieces[q].wait()
        here = slice(q * part, q * part + part)
        high, low = split(x_ref[here, :])
        high_ref[here, :], low_ref[here, :] = high, low
        a, b = bdot(high[:, :256], high[:, :256], TN), bdot(high[:, :256], low[:, :256], TN)
        one, two = (a, b) if one is None else (one + a, two + b)
    pack(0, one + two + two.T, out_ref)


def gram_second(high_ref, low_ref, out_ref):
    left, right = high_ref[:, :256], high_ref[:, 256:]
    pack(1, bdot(left, right, TN) + bdot(left, low_ref[:, 256:], TN) + bdot(low_ref[:, :256], right, TN), out_ref)


def gram_third(high_ref, low_ref, out_ref):
    both = bdot(high_ref[:, 256:], jnp.concatenate([high_ref[:, 256:], low_ref[:, 256:]], axis=1), TN)
    pack(2, both[:, :256] + both[:, 256:] + both[:, 256:].T, out_ref)


def gram_kernel(x_hbm, out_ref, x_ref, high_ref, low_ref, part_ref, x_sem, *scratch):
    work = StagedSum(part_ref, out_ref, *scratch)
    peers = [work.mate] + [peer for _, peer in work.along_y + work.along_z]
    x_pieces = pieces_in(x_hbm, x_ref, x_sem)
    greet(peers)
    gram_first(x_pieces, x_ref, high_ref, low_ref, part_ref)
    meet(peers)
    work.begin(0)
    gram_second(high_ref, low_ref, part_ref)
    work.begin(1)
    gram_third(high_ref, low_ref, part_ref)
    work.begin(2)
    work.finish()


def gram_over_rows(snapshots, number):
    rows = snapshots.shape[0]
    return pl.pallas_call(
        gram_kernel,
        in_specs=[pl.BlockSpec(memory_space=pl.ANY)],
        out_specs=VMEM,
        out_shape=jax.ShapeDtypeStruct((GRAM_ROWS, 128), F32),
        scratch_shapes=[
            pltpu.VMEM((rows, 512), F32),
            pltpu.VMEM((rows, 512), BF16),
            pltpu.VMEM((rows, 512), BF16),
            pltpu.VMEM((GRAM_ROWS, 128), F32),
            pltpu.SemaphoreType.DMA((4,)),
        ] + sum_scratch(GRAM_ROWS // 512),
        compiler_params=pltpu.CompilerParams(
            collective_id=number, has_side_effects=True, vmem_limit_bytes=48 * 1024 * 1024
        ),
        name="gram_over_rows",
    )(snapshots)


def solve_kernel(row_total, gram_ref, start_ref, out_ref, gram):
    for at, (i, j) in enumerate(((0, 0), (0, 1), (1, 1))):
        for h in range(2):
            block = gram_ref[512 * at + 256 * h : 512 * at + 256 * h + 256, :] * (1.0 / row_total)
            gram[256 * i : 256 * i + 256, 256 * j + 128 * h : 256 * j + 128 * h + 128] = block
    gram[256:512, 0:256] = gram[0:256, 256:512].T
    parts = split3(gram[...])
    block, ratio = orth_rows(times(times(times(start_ref[...], parts), parts), parts))
    block, last_ratio = orth_rows(times(times(times(block, parts), parts), parts))
    block, error = corrected(block, block)
    out_ref[...] = block
    fine = jnp.logical_and(jnp.minimum(ratio, last_ratio) > 3e-6, error < 1e-5)

    @pl.when(jnp.logical_not(fine))
    def _():
        step_by_step(start_ref[...], parts, out_ref)


def group_solve(gram, start_block, row_total):
    return pl.pallas_call(
        functools.partial(solve_kernel, row_total),
        in_specs=[VMEM, VMEM],
        out_specs=VMEM,
        out_shape=jax.ShapeDtypeStruct((RANK, 512), F32),
        scratch_shapes=[pltpu.VMEM((512, 512), F32)],
        compiler_params=pltpu.CompilerParams(vmem_limit_bytes=16 * 1024 * 1024),
        name="group_solve",
    )(gram, start_block)


PIECES = 4


def merge_products(q, joined_ref, test_ref, first, second, third):
    part = test_ref.shape[0] // PIECES
    high, low = split(joined_ref[:, q * part : (q + 1) * part])
    test_high, test_low = split(test_ref[q * part : (q + 1) * part, :])
    one = bdot(high, high, NT)
    two = bdot(high, low, NT)
    three = bdot(high, test_high, NN) + bdot(high, test_low, NN) + bdot(low, test_high, NN)
    if q == 0:
        first[...], second[...], third[...] = one, two, three
    else:
        first[...] = first[...] + one
        second[...] = second[...] + two
        third[...] = third[...] + three


def basis_piece(high_low, x):
    high, low = split(x)
    both = bdot(high_low, high, NT)
    return both[:RANK] + both[RANK:] + bdot(high_low[:RANK], low, NT)


def merge_kernel(
    iterate_ref, x_hbm, test_ref, out_ref, merge_ref, x_ref, part_ref, first, second, third, x_sem, send_g, recv_g, *scratch
):
    g = lax.axis_index("grp")
    y, z, c = (lax.axis_index(name) for name in ROW)
    right, left = lax.rem(g + 1, 4), lax.rem(g + 3, 4)
    part = x_ref.shape[0] // PIECES
    x_pieces = pieces_in(x_hbm, x_ref, x_sem)
    work = StagedSum(part_ref, merge_ref, *scratch)
    peers = [(right, y, z, c), (left, y, z, c), work.mate] + [peer for _, peer in work.along_y + work.along_z]
    greet(peers)
    high_low = jnp.concatenate(split(iterate_ref[...]), axis=0)

    def place(block, q, first_row, size):
        return out_ref.at[rows_at(block * RANK + first_row, size), pl.ds(q * part, part)]

    def own(q):
        return [
            remote(place(g, q, 0, RANK), place(g, q, 0, RANK), send_g.at[k, q], recv_g.at[k, q], (peer, y, z, c))
            for k, peer in enumerate((right, left))
        ]

    def on(q):
        return [
            remote(place(block, q, at, 32), place(block, q, at, 32), send_g.at[k, q], recv_g.at[k, q], (peer, y, z, c))
            for k, block, at, peer in ((2, left, 0, right), (3, right, 32, left))
        ]

    owns, ons = [own(q) for q in range(PIECES)], [on(q) for q in range(PIECES)]

    def start(made):
        for one in made:
            one.start()

    def arrived(made):
        for one in made:
            one.wait_recv()

    def make(q):
        x_pieces[q].wait()
        out_ref[rows_at(g * RANK, RANK), q * part : (q + 1) * part] = basis_piece(
            high_low, x_ref[q * part : (q + 1) * part, :]
        )

    make(0)
    meet(peers)
    start(owns[0])
    make(1)
    start(owns[1])
    make(2)
    for q in range(PIECES):
        arrived(owns[q])
        start(ons[q])
        if q + 2 < PIECES:
            start(owns[q + 2])
        if q + 3 < PIECES:
            make(q + 3)
        if q > 0:
            arrived(ons[q - 1])
            merge_products(q - 1, out_ref, test_ref, first, second, third)
    arrived(ons[PIECES - 1])
    merge_products(PIECES - 1, out_ref, test_ref, first, second, third)
    merged = first[...] + second[...] + second[...].T
    for h in range(2):
        part_ref[256 * h : 256 * h + 256, :] = merged[:, 128 * h : 128 * h + 128]
    work.begin(0)
    part_ref[512:768, :] = third[...]
    part_ref[768:, :] = jnp.zeros((MERGE_ROWS - 768, 128), F32)
    work.begin(1)
    work.finish()
    for made in owns + ons:
        for one in made:
            one.wait_send()


def merged_over_rows(iterate, snapshots, test_block, number):
    rows = snapshots.shape[0]
    dma = pltpu.SemaphoreType.DMA
    return pl.pallas_call(
        merge_kernel,
        in_specs=[VMEM, pl.BlockSpec(memory_space=pl.ANY), VMEM],
        out_specs=[VMEM, VMEM],
        out_shape=[jax.ShapeDtypeStruct((4 * RANK, rows), F32), jax.ShapeDtypeStruct((MERGE_ROWS, 128), F32)],
        scratch_shapes=[
            pltpu.VMEM((rows, 512), F32),
            pltpu.VMEM((MERGE_ROWS, 128), F32),
            pltpu.VMEM((256, 256), F32),
            pltpu.VMEM((256, 256), F32),
            pltpu.VMEM((256, 128), F32),
            dma((PIECES,)),
            dma((4, PIECES)),
            dma((4, PIECES)),
        ] + sum_scratch(MERGE_ROWS // 512),
        compiler_params=pltpu.CompilerParams(
            collective_id=number, has_side_effects=True, vmem_limit_bytes=48 * 1024 * 1024
        ),
        name="merged_over_rows",
    )(iterate, snapshots, test_block)


def project_kernel(row_total, merge_ref, start_ref, joined_ref, out_ref, merged, coef_ref, factor):
    @pl.when(pl.program_id(0) == 0)
    def _():
        for h in range(2):
            merged[:, 128 * h : 128 * h + 128] = merge_ref[256 * h : 256 * h + 256, :] * (1.0 / row_total)
        parts = split3(merged[...])

        def to_modes(block):
            inverse, _, _ = lower_inverse(fdot(times(block, parts), block, NT))
            block = fdot(inverse, block)
            return corrected(block, times(block, parts))

        block, ratio = orth_rows(times(times(start_ref[...], parts), parts))
        block, next_ratio = orth_rows(times(times(block, parts), parts))
        coef, error = to_modes(times(times(block, parts), parts))
        coef_ref[...] = coef
        fine = jnp.logical_and(jnp.minimum(ratio, next_ratio) > 3e-6, error < 1e-4)

        @pl.when(jnp.logical_not(fine))
        def _():
            step_by_step(start_ref[...], parts, coef_ref)
            coef_ref[...] = to_modes(coef_ref[...])[0]

        coef = coef_ref[...]
        test_coeffs = fdot(coef, merge_ref[512:768, :]) * (1.0 / row_total)
        high, low = split(fdot(test_coeffs, coef, TN))
        factor[0:128, :] = high
        factor[128:, :] = low

    size = out_ref.shape[0]
    here = pl.ds(pl.multiple_of(pl.program_id(0) * size, 128), size)
    high, low = split(joined_ref[:, here])
    both = bdot(factor[...], high, NN)
    out_ref[...] = (both[:128] + both[128:] + bdot(factor[0:128, :], low, NN)).T


def project(merge, start_merge, joined, row_total):
    rows = joined.shape[1]
    return pl.pallas_call(
        functools.partial(project_kernel, row_total),
        grid=(rows // 512,),
        in_specs=[VMEM, VMEM, VMEM],
        out_specs=pl.BlockSpec((512, 128), lambda i: (i, 0)),
        out_shape=jax.ShapeDtypeStruct((rows, 128), F32),
        scratch_shapes=[pltpu.VMEM((256, 256), F32), pltpu.VMEM((RANK, 256), F32), pltpu.VMEM((256, 256), BF16)],
        compiler_params=pltpu.CompilerParams(vmem_limit_bytes=16 * 1024 * 1024),
        name="project",
    )(merge, start_merge, joined)


def on_device(snapshots, test_block, start_block, start_merge):
    row_total = snapshots.shape[0] * 64
    gram = gram_over_rows(snapshots, 0)
    iterate = group_solve(gram, start_block.T, row_total)
    joined, merge = merged_over_rows(iterate, snapshots, test_block, 1)
    return project(merge, start_merge.T, joined, row_total)


def solution(mesh):
    finer = Mesh(
        mesh.devices.reshape(mesh.shape["grp"], 4, 8, 2), ("grp", "row_0", "row_1", "row_2")
    )
    placed = (P(ROW, "grp"), P(ROW, "grp"), P("grp", None), P())
    return jax.shard_map(
        on_device, mesh=finer, in_specs=placed, out_specs=P(ROW, "grp"), check_vma=False
    )
```

```python
import functools

import jax
import jax.numpy as jnp
from jax import lax
from jax.experimental import pallas as pl
from jax.experimental.pallas import tpu as pltpu
from jax.sharding import Mesh
from jax.sharding import PartitionSpec as P

ITERS = 6
RANK = 64
ROW = ("row_0", "row_1", "row_2")
MESH = pl.DeviceIdType.MESH
F32, BF16 = jnp.float32, jnp.bfloat16
NT = (((1,), (1,)), ((), ()))
TN = (((0,), (0,)), ((), ()))
NN = (((1,), (0,)), ((), ()))
VMEM = pl.BlockSpec(memory_space=pltpu.VMEM)
GRAM_ROWS = 1536
MERGE_ROWS = 1024


def split(x):
    high = x.astype(BF16)
    return high, (x - high.astype(F32)).astype(BF16)


def bdot(a, b, dims):
    return lax.dot_general(a, b, dims, preferred_element_type=F32)


def fdot(a, b, dims=NN):
    return lax.dot_general(
        a, b, dims, precision=lax.Precision.HIGHEST, preferred_element_type=F32
    )


def spread(x):
    return jnp.broadcast_to(x, (8, 128))


def lower_inverse(small):
    rows8 = lax.broadcasted_iota(jnp.int32, (8, 128), 0)
    row, lane = (lax.broadcasted_iota(jnp.int32, (64, 64), d) for d in (0, 1))
    joint = jnp.concatenate([jnp.where(row == lane, 1.0, 0.0), small], axis=1)
    bands = [joint[8 * k : 8 * k + 8, :] for k in range(8)]
    done, least, most = [], None, None
    corner = [spread(bands[0][:, 64 + c : 65 + c]) for c in range(8)]
    for k in range(8):
        first = 64 + 8 * k
        cols = [corner]
        cols += [[spread(bands[i][:, first + c : first + c + 1]) for c in range(8)] for i in range(k + 1, 8)]
        if k < 7:
            corner = [spread(bands[k + 1][:, first + 8 + c : first + 9 + c]) for c in range(8)]
        line = [spread(bands[k][a : a + 1, :]) for a in range(8)]
        piv = [[spread(cols[0][c][a : a + 1, :]) for c in range(a + 1)] for a in range(8)]
        for a in range(8):
            inv = 1.0 / piv[a][a]
            low = {c: piv[c][a] * inv for c in range(a + 1, 8)}
            for c in range(a + 1, 8):
                for e in range(a + 1, c + 1):
                    piv[c][e] = piv[c][e] - low[c] * piv[e][a]
            for c in range(a + 1, 8):
                line[c] = line[c] - low[c] * line[a]
            for i in range(1, 8 - k):
                share = cols[i][a] * inv
                bands[k + i] = bands[k + i] - share * line[a]
                if i == 1:
                    corner = [corner[c] - share * spread(cols[1][a][c : c + 1, :]) for c in range(8)]
                for c in range(a + 1, 8):
                    cols[i][c] = cols[i][c] - share * piv[c][a]
        band, diag = line[0], piv[0][0]
        for a in range(1, 8):
            band = jnp.where(rows8 == a, line[a], band)
            diag = jnp.where(rows8 == a, piv[a][a], diag)
        done.append(band * lax.rsqrt(diag))
        least = diag if least is None else jnp.minimum(least, diag)
        most = diag if most is None else jnp.maximum(most, diag)
    return jnp.concatenate(done, axis=0)[:, :64], jnp.min(least), jnp.max(most)


def split3(x):
    high = x.astype(BF16)
    rest = x - high.astype(F32)
    mid = rest.astype(BF16)
    return high, mid, (rest - mid.astype(F32)).astype(BF16)


def times(block, parts):
    three = jnp.concatenate(split3(block), axis=0)
    n = block.shape[0]
    one = bdot(three, parts[0], NN)
    two = bdot(three[: 2 * n], parts[1], NN)
    low = one[2 * n :] + two[n:] + bdot(three[:n], parts[2], NN)
    return one[:n] + ((one[n : 2 * n] + two[:n]) + low)


def orth_rows(block):
    inverse, least, most = lower_inverse(fdot(block, block, NT))
    return fdot(inverse, block), least / most


def corrected(block, images):
    row, lane = (lax.broadcasted_iota(jnp.int32, (RANK, RANK), d) for d in (0, 1))
    excess = fdot(block, images, NT) - jnp.where(row == lane, 1.0, 0.0)
    part = jnp.where(row > lane, excess, jnp.where(row == lane, 0.5 * excess, 0.0))
    return block - fdot(part, block), jnp.sum(excess * excess)


def step_by_step(start, parts, out_ref):
    out_ref[...] = orth_rows(start)[0]

    def one(_, carry):
        out_ref[...] = orth_rows(times(out_ref[...], parts))[0]
        return carry

    lax.fori_loop(0, ITERS, one, 0)


def rows_at(start, size):
    return pl.ds(pl.multiple_of(start, 8), size)


def remote(src, dst, send, recv, device):
    return pltpu.make_async_remote_copy(
        src_ref=src, dst_ref=dst, send_sem=send, recv_sem=recv, device_id=device, device_id_type=MESH
    )


def row_peers():
    grp = lax.axis_index("grp")
    y, z, c = (lax.axis_index(name) for name in ROW)
    along_y = [(lax.rem(y + d, 4), (grp, lax.rem(y + d, 4), z, c)) for d in range(1, 4)]
    along_z = [(lax.rem(z + d, 8), (grp, y, lax.rem(z + d, 8), c)) for d in range(1, 8)]
    return (grp, y, z, 1 - c), along_y, along_z


def greet(peers):
    barrier = pltpu.get_barrier_semaphore()
    for peer in peers:
        pl.semaphore_signal(barrier, inc=1, device_id=peer, device_id_type=MESH)


def meet(peers):
    pl.semaphore_wait(pltpu.get_barrier_semaphore(), len(peers))


def pieces_in(src, dst, sem, cuts):
    made = [
        pltpu.make_async_copy(src.at[pl.ds(at, size)], dst.at[pl.ds(at, size)], sem.at[q])
        for q, (at, size) in enumerate(cuts)
    ]
    for one in made:
        one.start()
    return made


class StagedSum:
    def __init__(self, in_ref, out_ref, got1, sum1, got2, sum2, got3, send, recv):
        self.in_ref, self.out_ref = in_ref, out_ref
        self.got1, self.sum1, self.got2, self.sum2, self.got3 = got1, sum1, got2, sum2, got3
        self.send, self.recv = send, recv
        self.stage, self.flying = {}, {}
        self.mate, self.along_y, self.along_z = row_peers()
        self.y, self.z, self.c = (lax.axis_index(name) for name in ROW)

    def copy(self, i, at, src, dst, device):
        return remote(src, dst, self.send.at[i, at], self.recv.at[i, at], device)

    def halves(self, i):
        src = self.in_ref.at[rows_at(512 * i + (1 - self.c) * 256, 256)]
        return [self.copy(i, 0, src, self.got1.at[i], self.mate)]

    def quarters(self, i):
        return [
            self.copy(i, 1 + d, self.sum1.at[i, rows_at(y * 64, 64)], self.got2.at[i, d], peer)
            for d, (y, peer) in enumerate(self.along_y)
        ]

    def eighths(self, i):
        return [
            self.copy(i, 4 + d, self.sum2.at[i, rows_at(z * 8, 8)], self.got3.at[i, d], peer)
            for d, (z, peer) in enumerate(self.along_z)
        ]

    def back_z(self, i):
        mine = self.out_ref.at[rows_at(512 * i + self.c * 256 + self.y * 64 + self.z * 8, 8)]
        return [self.copy(i, 11 + d, mine, mine, peer) for d, (_, peer) in enumerate(self.along_z)]

    def back_y(self, i):
        mine = self.out_ref.at[rows_at(512 * i + self.c * 256 + self.y * 64, 64)]
        return [self.copy(i, 18 + d, mine, mine, peer) for d, (_, peer) in enumerate(self.along_y)]

    def back_core(self, i):
        mine = self.out_ref.at[rows_at(512 * i + self.c * 256, 256)]
        return [self.copy(i, 21, mine, mine, self.mate)]

    def add(self, stage, i):
        if stage == 0:
            self.sum1[i] = self.in_ref[rows_at(512 * i + self.c * 256, 256), :] + self.got1[i]
        elif stage == 1:
            self.sum2[i] = self.sum1[i, rows_at(self.y * 64, 64), :] + self.got2[i, 0] + self.got2[i, 1] + self.got2[i, 2]
        elif stage == 2:
            total = self.sum2[i, rows_at(self.z * 8, 8), :]
            for d in range(7):
                total = total + self.got3[i, d]
            self.out_ref[rows_at(512 * i + self.c * 256 + self.y * 64 + self.z * 8, 8), :] = total

    def begin(self, i):
        self.stage[i], self.flying[i] = 0, self.halves(i)
        for one in self.flying[i]:
            one.start()

    def advance(self, i):
        for one in self.flying[i]:
            one.wait()
        stage = self.stage[i]
        self.add(stage, i)
        self.stage[i] = stage + 1
        if stage < 5:
            following = (self.quarters, self.eighths, self.back_z, self.back_y, self.back_core)[stage]
            self.flying[i] = following(i)
            for one in self.flying[i]:
                one.start()

    def finish(self):
        while min(self.stage.values()) < 6:
            low = min(self.stage.values())
            for i in sorted(self.stage):
                if self.stage[i] == low:
                    self.advance(i)


def sum_scratch(chunks):
    dma = pltpu.SemaphoreType.DMA
    return [
        pltpu.VMEM((chunks, 256, 128), F32),
        pltpu.VMEM((chunks, 256, 128), F32),
        pltpu.VMEM((chunks, 3, 64, 128), F32),
        pltpu.VMEM((chunks, 64, 128), F32),
        pltpu.VMEM((chunks, 7, 8, 128), F32),
        dma((chunks, 22)),
        dma((chunks, 22)),
    ]


def pack(at, block, out_ref):
    for h in range(2):
        out_ref[512 * at + 256 * h : 512 * at + 256 * h + 256, :] = block[:, 128 * h : 128 * h + 128]


def gram_first(x_pieces, x_ref, high_ref, low_ref, out_ref):
    part = x_ref.shape[0] // 4
    one = two = None
    for q in range(4):
        x_pieces[q].wait()
        here = slice(q * part, q * part + part)
        high, low = split(x_ref[here, :])
        high_ref[here, :], low_ref[here, :] = high, low
        a, b = bdot(high[:, :256], high[:, :256], TN), bdot(high[:, :256], low[:, :256], TN)
        one, two = (a, b) if one is None else (one + a, two + b)
    pack(0, one + two + two.T, out_ref)


def gram_second(high_ref, low_ref, out_ref):
    left, right = high_ref[:, :256], high_ref[:, 256:]
    pack(1, bdot(left, right, TN) + bdot(left, low_ref[:, 256:], TN) + bdot(low_ref[:, :256], right, TN), out_ref)


def gram_third(high_ref, low_ref, out_ref):
    both = bdot(high_ref[:, 256:], jnp.concatenate([high_ref[:, 256:], low_ref[:, 256:]], axis=1), TN)
    pack(2, both[:, :256] + both[:, 256:] + both[:, 256:].T, out_ref)


def gram_kernel(x_hbm, out_ref, x_ref, high_ref, low_ref, part_ref, x_sem, *scratch):
    work = StagedSum(part_ref, out_ref, *scratch)
    peers = [work.mate] + [peer for _, peer in work.along_y + work.along_z]
    part = x_ref.shape[0] // 4
    x_pieces = pieces_in(x_hbm, x_ref, x_sem, [(q * part, part) for q in range(4)])
    greet(peers)
    gram_first(x_pieces, x_ref, high_ref, low_ref, part_ref)
    meet(peers)
    work.begin(0)
    gram_second(high_ref, low_ref, part_ref)
    work.begin(1)
    gram_third(high_ref, low_ref, part_ref)
    work.begin(2)
    work.finish()


def gram_over_rows(snapshots, number):
    rows = snapshots.shape[0]
    return pl.pallas_call(
        gram_kernel,
        in_specs=[pl.BlockSpec(memory_space=pl.ANY)],
        out_specs=VMEM,
        out_shape=jax.ShapeDtypeStruct((GRAM_ROWS, 128), F32),
        scratch_shapes=[
            pltpu.VMEM((rows, 512), F32),
            pltpu.VMEM((rows, 512), BF16),
            pltpu.VMEM((rows, 512), BF16),
            pltpu.VMEM((GRAM_ROWS, 128), F32),
            pltpu.SemaphoreType.DMA((4,)),
        ] + sum_scratch(GRAM_ROWS // 512),
        compiler_params=pltpu.CompilerParams(
            collective_id=number, has_side_effects=True, vmem_limit_bytes=48 * 1024 * 1024
        ),
        name="gram_over_rows",
    )(snapshots)


def solve_kernel(row_total, gram_ref, start_ref, out_ref, gram):
    for at, (i, j) in enumerate(((0, 0), (0, 1), (1, 1))):
        for h in range(2):
            block = gram_ref[512 * at + 256 * h : 512 * at + 256 * h + 256, :] * (1.0 / row_total)
            gram[256 * i : 256 * i + 256, 256 * j + 128 * h : 256 * j + 128 * h + 128] = block
    gram[256:512, 0:256] = gram[0:256, 256:512].T
    parts = split3(gram[...])
    block, ratio = orth_rows(times(times(times(start_ref[...], parts), parts), parts))
    block, last_ratio = orth_rows(times(times(times(block, parts), parts), parts))
    block, error = corrected(block, block)
    out_ref[...] = block
    fine = jnp.logical_and(jnp.minimum(ratio, last_ratio) > 3e-6, error < 1e-5)

    @pl.when(jnp.logical_not(fine))
    def _():
        step_by_step(start_ref[...], parts, out_ref)


def group_solve(gram, start_block, row_total):
    return pl.pallas_call(
        functools.partial(solve_kernel, row_total),
        in_specs=[VMEM, VMEM],
        out_specs=VMEM,
        out_shape=jax.ShapeDtypeStruct((RANK, 512), F32),
        scratch_shapes=[pltpu.VMEM((512, 512), F32)],
        compiler_params=pltpu.CompilerParams(vmem_limit_bytes=16 * 1024 * 1024),
        name="group_solve",
    )(gram, start_block)


SHARES = (4, 7, 7, 7, 3)
PIECES = len(SHARES)


def row_cuts(rows):
    unit = rows // sum(SHARES)
    return [(unit * sum(SHARES[:q]), unit * SHARES[q]) for q in range(PIECES)]


def merge_products(q, joined_ref, test_ref, first, second, third):
    at, size = row_cuts(test_ref.shape[0])[q]
    high, low = split(joined_ref[:, at : at + size])
    test_high, test_low = split(test_ref[at : at + size, :])
    one = bdot(high, high, NT)
    two = bdot(high, low, NT)
    three = bdot(high, test_high, NN) + bdot(high, test_low, NN) + bdot(low, test_high, NN)
    if q == 0:
        first[...], second[...], third[...] = one, two, three
    else:
        first[...] = first[...] + one
        second[...] = second[...] + two
        third[...] = third[...] + three


def basis_piece(high_low, x):
    high, low = split(x)
    both = bdot(high_low, high, NT)
    return both[:RANK] + both[RANK:] + bdot(high_low[:RANK], low, NT)


def merge_kernel(
    iterate_ref, x_hbm, test_ref, out_ref, merge_ref, x_ref, part_ref, first, second, third, x_sem, send_g, recv_g, *scratch
):
    g = lax.axis_index("grp")
    y, z, c = (lax.axis_index(name) for name in ROW)
    right, left = lax.rem(g + 1, 4), lax.rem(g + 3, 4)
    cuts = row_cuts(x_ref.shape[0])
    x_pieces = pieces_in(x_hbm, x_ref, x_sem, cuts)
    work = StagedSum(part_ref, merge_ref, *scratch)
    peers = [(right, y, z, c), (left, y, z, c), work.mate] + [peer for _, peer in work.along_y + work.along_z]
    greet(peers)
    high_low = jnp.concatenate(split(iterate_ref[...]), axis=0)

    def place(block, q, first_row, size):
        return out_ref.at[rows_at(block * RANK + first_row, size), pl.ds(*cuts[q])]

    def own(q):
        return [
            remote(place(g, q, 0, RANK), place(g, q, 0, RANK), send_g.at[k, q], recv_g.at[k, q], (peer, y, z, c))
            for k, peer in enumerate((right, left))
        ]

    def on(q):
        return [
            remote(place(block, q, at, 32), place(block, q, at, 32), send_g.at[k, q], recv_g.at[k, q], (peer, y, z, c))
            for k, block, at, peer in ((2, left, 0, right), (3, right, 32, left))
        ]

    owns, ons = [own(q) for q in range(PIECES)], [on(q) for q in range(PIECES)]

    def start(made):
        for one in made:
            one.start()

    def arrived(made):
        for one in made:
            one.wait_recv()

    def make(q):
        x_pieces[q].wait()
        at, size = cuts[q]
        out_ref[rows_at(g * RANK, RANK), at : at + size] = basis_piece(high_low, x_ref[at : at + size, :])

    make(0)
    meet(peers)
    start(owns[0])
    make(1)
    start(owns[1])
    make(2)
    for q in range(PIECES):
        arrived(owns[q])
        start(ons[q])
        if q + 2 < PIECES:
            start(owns[q + 2])
        if q + 3 < PIECES:
            make(q + 3)
        if q > 0:
            arrived(ons[q - 1])
            merge_products(q - 1, out_ref, test_ref, first, second, third)
    arrived(ons[PIECES - 1])
    merge_products(PIECES - 1, out_ref, test_ref, first, second, third)
    merged = first[...] + second[...] + second[...].T
    for h in range(2):
        part_ref[256 * h : 256 * h + 256, :] = merged[:, 128 * h : 128 * h + 128]
    work.begin(0)
    part_ref[512:768, :] = third[...]
    part_ref[768:, :] = jnp.zeros((MERGE_ROWS - 768, 128), F32)
    work.begin(1)
    work.finish()
    for made in owns + ons:
        for one in made:
            one.wait_send()


def merged_over_rows(iterate, snapshots, test_block, number):
    rows = snapshots.shape[0]
    dma = pltpu.SemaphoreType.DMA
    return pl.pallas_call(
        merge_kernel,
        in_specs=[VMEM, pl.BlockSpec(memory_space=pl.ANY), VMEM],
        out_specs=[VMEM, VMEM],
        out_shape=[jax.ShapeDtypeStruct((4 * RANK, rows), F32), jax.ShapeDtypeStruct((MERGE_ROWS, 128), F32)],
        scratch_shapes=[
            pltpu.VMEM((rows, 512), F32),
            pltpu.VMEM((MERGE_ROWS, 128), F32),
            pltpu.VMEM((256, 256), F32),
            pltpu.VMEM((256, 256), F32),
            pltpu.VMEM((256, 128), F32),
            dma((PIECES,)),
            dma((4, PIECES)),
            dma((4, PIECES)),
        ] + sum_scratch(MERGE_ROWS // 512),
        compiler_params=pltpu.CompilerParams(
            collective_id=number, has_side_effects=True, vmem_limit_bytes=48 * 1024 * 1024
        ),
        name="merged_over_rows",
    )(iterate, snapshots, test_block)


def project_kernel(row_total, merge_ref, start_ref, joined_ref, out_ref, merged, coef_ref, factor):
    @pl.when(pl.program_id(0) == 0)
    def _():
        for h in range(2):
            merged[:, 128 * h : 128 * h + 128] = merge_ref[256 * h : 256 * h + 256, :] * (1.0 / row_total)
        parts = split3(merged[...])

        def to_modes(block):
            inverse, _, _ = lower_inverse(fdot(times(block, parts), block, NT))
            block = fdot(inverse, block)
            return corrected(block, times(block, parts))

        block, ratio = orth_rows(times(times(start_ref[...], parts), parts))
        block, next_ratio = orth_rows(times(times(block, parts), parts))
        coef, error = to_modes(times(times(block, parts), parts))
        coef_ref[...] = coef
        fine = jnp.logical_and(jnp.minimum(ratio, next_ratio) > 3e-6, error < 1e-4)

        @pl.when(jnp.logical_not(fine))
        def _():
            step_by_step(start_ref[...], parts, coef_ref)
            coef_ref[...] = to_modes(coef_ref[...])[0]

        coef = coef_ref[...]
        test_coeffs = fdot(coef, merge_ref[512:768, :]) * (1.0 / row_total)
        high, low = split(fdot(test_coeffs, coef, TN))
        factor[0:128, :] = high
        factor[128:, :] = low

    size = out_ref.shape[0]
    here = pl.ds(pl.multiple_of(pl.program_id(0) * size, 128), size)
    high, low = split(joined_ref[:, here])
    both = bdot(factor[...], high, NN)
    out_ref[...] = (both[:128] + both[128:] + bdot(factor[0:128, :], low, NN)).T


def project(merge, start_merge, joined, row_total):
    rows = joined.shape[1]
    return pl.pallas_call(
        functools.partial(project_kernel, row_total),
        grid=(rows // 512,),
        in_specs=[VMEM, VMEM, VMEM],
        out_specs=pl.BlockSpec((512, 128), lambda i: (i, 0)),
        out_shape=jax.ShapeDtypeStruct((rows, 128), F32),
        scratch_shapes=[pltpu.VMEM((256, 256), F32), pltpu.VMEM((RANK, 256), F32), pltpu.VMEM((256, 256), BF16)],
        compiler_params=pltpu.CompilerParams(vmem_limit_bytes=16 * 1024 * 1024),
        name="project",
    )(merge, start_merge, joined)


def on_device(snapshots, test_block, start_block, start_merge):
    row_total = snapshots.shape[0] * 64
    gram = gram_over_rows(snapshots, 0)
    iterate = group_solve(gram, start_block.T, row_total)
    joined, merge = merged_over_rows(iterate, snapshots, test_block, 1)
    return project(merge, start_merge.T, joined, row_total)


def solution(mesh):
    finer = Mesh(
        mesh.devices.reshape(mesh.shape["grp"], 4, 8, 2), ("grp", "row_0", "row_1", "row_2")
    )
    placed = (P(ROW, "grp"), P(ROW, "grp"), P("grp", None), P())
    return jax.shard_map(
        on_device, mesh=finer, in_specs=placed, out_specs=P(ROW, "grp"), check_vma=False
    )
```

```python
import functools

import jax
import jax.numpy as jnp
from jax import lax
from jax.experimental import pallas as pl
from jax.experimental.pallas import tpu as pltpu
from jax.sharding import Mesh
from jax.sharding import PartitionSpec as P

ITERS = 6
RANK = 64
ROW = ("row_0", "row_1", "row_2")
MESH = pl.DeviceIdType.MESH
F32, BF16 = jnp.float32, jnp.bfloat16
NT = (((1,), (1,)), ((), ()))
TN = (((0,), (0,)), ((), ()))
NN = (((1,), (0,)), ((), ()))
VMEM = pl.BlockSpec(memory_space=pltpu.VMEM)
GRAM_ROWS = 1536
MERGE_ROWS = 1024


def split(x):
    high = x.astype(BF16)
    return high, (x - high.astype(F32)).astype(BF16)


def bdot(a, b, dims):
    return lax.dot_general(a, b, dims, preferred_element_type=F32)


def fdot(a, b, dims=NN):
    return lax.dot_general(
        a, b, dims, precision=lax.Precision.HIGHEST, preferred_element_type=F32
    )


def spread(x):
    return jnp.broadcast_to(x, (8, 128))


def lower_inverse(small):
    rows8 = lax.broadcasted_iota(jnp.int32, (8, 128), 0)
    row, lane = (lax.broadcasted_iota(jnp.int32, (64, 64), d) for d in (0, 1))
    joint = jnp.concatenate([jnp.where(row == lane, 1.0, 0.0), small], axis=1)
    bands = [joint[8 * k : 8 * k + 8, :] for k in range(8)]
    done, least, most = [], None, None
    corner = [spread(bands[0][:, 64 + c : 65 + c]) for c in range(8)]
    for k in range(8):
        first = 64 + 8 * k
        cols = [corner]
        cols += [[spread(bands[i][:, first + c : first + c + 1]) for c in range(8)] for i in range(k + 1, 8)]
        if k < 7:
            corner = [spread(bands[k + 1][:, first + 8 + c : first + 9 + c]) for c in range(8)]
        line = [spread(bands[k][a : a + 1, :]) for a in range(8)]
        piv = [[spread(cols[0][c][a : a + 1, :]) for c in range(a + 1)] for a in range(8)]
        for a in range(8):
            inv = 1.0 / piv[a][a]
            low = {c: piv[c][a] * inv for c in range(a + 1, 8)}
            for c in range(a + 1, 8):
                for e in range(a + 1, c + 1):
                    piv[c][e] = piv[c][e] - low[c] * piv[e][a]
            for c in range(a + 1, 8):
                line[c] = line[c] - low[c] * line[a]
            for i in range(1, 8 - k):
                share = cols[i][a] * inv
                bands[k + i] = bands[k + i] - share * line[a]
                if i == 1:
                    corner = [corner[c] - share * spread(cols[1][a][c : c + 1, :]) for c in range(8)]
                for c in range(a + 1, 8):
                    cols[i][c] = cols[i][c] - share * piv[c][a]
        band, diag = line[0], piv[0][0]
        for a in range(1, 8):
            band = jnp.where(rows8 == a, line[a], band)
            diag = jnp.where(rows8 == a, piv[a][a], diag)
        done.append(band * lax.rsqrt(diag))
        least = diag if least is None else jnp.minimum(least, diag)
        most = diag if most is None else jnp.maximum(most, diag)
    return jnp.concatenate(done, axis=0)[:, :64], jnp.min(least), jnp.max(most)


def split3(x):
    high = x.astype(BF16)
    rest = x - high.astype(F32)
    mid = rest.astype(BF16)
    return high, mid, (rest - mid.astype(F32)).astype(BF16)


def times(block, parts):
    three = jnp.concatenate(split3(block), axis=0)
    n = block.shape[0]
    one = bdot(three, parts[0], NN)
    two = bdot(three[: 2 * n], parts[1], NN)
    low = one[2 * n :] + two[n:] + bdot(three[:n], parts[2], NN)
    return one[:n] + ((one[n : 2 * n] + two[:n]) + low)


def orth_rows(block):
    inverse, least, most = lower_inverse(fdot(block, block, NT))
    return fdot(inverse, block), least / most


def corrected(block, images):
    row, lane = (lax.broadcasted_iota(jnp.int32, (RANK, RANK), d) for d in (0, 1))
    excess = fdot(block, images, NT) - jnp.where(row == lane, 1.0, 0.0)
    part = jnp.where(row > lane, excess, jnp.where(row == lane, 0.5 * excess, 0.0))
    return block - fdot(part, block), jnp.sum(excess * excess)


def step_by_step(start, parts, out_ref):
    out_ref[...] = orth_rows(start)[0]

    def one(_, carry):
        out_ref[...] = orth_rows(times(out_ref[...], parts))[0]
        return carry

    lax.fori_loop(0, ITERS, one, 0)


def rows_at(start, size):
    return pl.ds(pl.multiple_of(start, 8), size)


def remote(src, dst, send, recv, device):
    return pltpu.make_async_remote_copy(
        src_ref=src, dst_ref=dst, send_sem=send, recv_sem=recv, device_id=device, device_id_type=MESH
    )


def row_peers():
    grp = lax.axis_index("grp")
    y, z, c = (lax.axis_index(name) for name in ROW)
    along_y = [(lax.rem(y + d, 4), (grp, lax.rem(y + d, 4), z, c)) for d in range(1, 4)]
    along_z = [(lax.rem(z + d, 8), (grp, y, lax.rem(z + d, 8), c)) for d in range(1, 8)]
    return (grp, y, z, 1 - c), along_y, along_z


def greet(peers):
    barrier = pltpu.get_barrier_semaphore()
    for peer in peers:
        pl.semaphore_signal(barrier, inc=1, device_id=peer, device_id_type=MESH)


def meet(peers):
    pl.semaphore_wait(pltpu.get_barrier_semaphore(), len(peers))


def pieces_in(src, dst, sem):
    count = sem.shape[0]
    part = src.shape[0] // count
    made = [
        pltpu.make_async_copy(src.at[pl.ds(q * part, part)], dst.at[pl.ds(q * part, part)], sem.at[q])
        for q in range(count)
    ]
    for one in made:
        one.start()
    return made


class StagedSum:
    def __init__(self, in_ref, out_ref, got1, sum1, got2, sum2, got3, send, recv):
        self.in_ref, self.out_ref = in_ref, out_ref
        self.got1, self.sum1, self.got2, self.sum2, self.got3 = got1, sum1, got2, sum2, got3
        self.send, self.recv = send, recv
        self.stage, self.flying = {}, {}
        self.mate, self.along_y, self.along_z = row_peers()
        self.y, self.z, self.c = (lax.axis_index(name) for name in ROW)

    def copy(self, i, at, src, dst, device):
        return remote(src, dst, self.send.at[i, at], self.recv.at[i, at], device)

    def halves(self, i):
        src = self.in_ref.at[rows_at(512 * i + (1 - self.c) * 256, 256)]
        return [self.copy(i, 0, src, self.got1.at[i], self.mate)]

    def quarters(self, i):
        return [
            self.copy(i, 1 + d, self.sum1.at[i, rows_at(y * 64, 64)], self.got2.at[i, d], peer)
            for d, (y, peer) in enumerate(self.along_y)
        ]

    def eighths(self, i):
        return [
            self.copy(i, 4 + d, self.sum2.at[i, rows_at(z * 8, 8)], self.got3.at[i, d], peer)
            for d, (z, peer) in enumerate(self.along_z)
        ]

    def back_z(self, i):
        mine = self.out_ref.at[rows_at(512 * i + self.c * 256 + self.y * 64 + self.z * 8, 8)]
        return [self.copy(i, 11 + d, mine, mine, peer) for d, (_, peer) in enumerate(self.along_z)]

    def back_y(self, i):
        mine = self.out_ref.at[rows_at(512 * i + self.c * 256 + self.y * 64, 64)]
        return [self.copy(i, 18 + d, mine, mine, peer) for d, (_, peer) in enumerate(self.along_y)]

    def back_core(self, i):
        mine = self.out_ref.at[rows_at(512 * i + self.c * 256, 256)]
        return [self.copy(i, 21, mine, mine, self.mate)]

    def add(self, stage, i):
        if stage == 0:
            self.sum1[i] = self.in_ref[rows_at(512 * i + self.c * 256, 256), :] + self.got1[i]
        elif stage == 1:
            self.sum2[i] = self.sum1[i, rows_at(self.y * 64, 64), :] + self.got2[i, 0] + self.got2[i, 1] + self.got2[i, 2]
        elif stage == 2:
            total = self.sum2[i, rows_at(self.z * 8, 8), :]
            for d in range(7):
                total = total + self.got3[i, d]
            self.out_ref[rows_at(512 * i + self.c * 256 + self.y * 64 + self.z * 8, 8), :] = total

    def begin(self, i):
        self.stage[i], self.flying[i] = 0, self.halves(i)
        for one in self.flying[i]:
            one.start()

    def advance(self, i):
        for one in self.flying[i]:
            one.wait()
        stage = self.stage[i]
        self.add(stage, i)
        self.stage[i] = stage + 1
        if stage < 5:
            following = (self.quarters, self.eighths, self.back_z, self.back_y, self.back_core)[stage]
            self.flying[i] = following(i)
            for one in self.flying[i]:
                one.start()

    def finish(self):
        while min(self.stage.values()) < 6:
            low = min(self.stage.values())
            for i in sorted(self.stage):
                if self.stage[i] == low:
                    self.advance(i)


def sum_scratch(chunks):
    dma = pltpu.SemaphoreType.DMA
    return [
        pltpu.VMEM((chunks, 256, 128), F32),
        pltpu.VMEM((chunks, 256, 128), F32),
        pltpu.VMEM((chunks, 3, 64, 128), F32),
        pltpu.VMEM((chunks, 64, 128), F32),
        pltpu.VMEM((chunks, 7, 8, 128), F32),
        dma((chunks, 22)),
        dma((chunks, 22)),
    ]


def pack(at, block, out_ref):
    for h in range(2):
        out_ref[512 * at + 256 * h : 512 * at + 256 * h + 256, :] = block[:, 128 * h : 128 * h + 128]


def gram_first(x_pieces, x_ref, high_ref, low_ref, out_ref):
    part = x_ref.shape[0] // 4
    one = two = None
    for q in range(4):
        x_pieces[q].wait()
        here = slice(q * part, q * part + part)
        high, low = split(x_ref[here, :])
        high_ref[here, :], low_ref[here, :] = high, low
        a, b = bdot(high[:, :256], high[:, :256], TN), bdot(high[:, :256], low[:, :256], TN)
        one, two = (a, b) if one is None else (one + a, two + b)
    pack(0, one + two + two.T, out_ref)


def gram_second(high_ref, low_ref, out_ref):
    left, right = high_ref[:, :256], high_ref[:, 256:]
    pack(1, bdot(left, right, TN) + bdot(left, low_ref[:, 256:], TN) + bdot(low_ref[:, :256], right, TN), out_ref)


def gram_third(high_ref, low_ref, out_ref):
    both = bdot(high_ref[:, 256:], jnp.concatenate([high_ref[:, 256:], low_ref[:, 256:]], axis=1), TN)
    pack(2, both[:, :256] + both[:, 256:] + both[:, 256:].T, out_ref)


def gram_kernel(x_hbm, out_ref, x_ref, high_ref, low_ref, part_ref, x_sem, *scratch):
    work = StagedSum(part_ref, out_ref, *scratch)
    peers = [work.mate] + [peer for _, peer in work.along_y + work.along_z]
    x_pieces = pieces_in(x_hbm, x_ref, x_sem)
    greet(peers)
    gram_first(x_pieces, x_ref, high_ref, low_ref, part_ref)
    meet(peers)
    work.begin(0)
    gram_second(high_ref, low_ref, part_ref)
    work.begin(1)
    gram_third(high_ref, low_ref, part_ref)
    work.begin(2)
    work.finish()


def gram_over_rows(snapshots, number):
    rows = snapshots.shape[0]
    return pl.pallas_call(
        gram_kernel,
        in_specs=[pl.BlockSpec(memory_space=pl.ANY)],
        out_specs=VMEM,
        out_shape=jax.ShapeDtypeStruct((GRAM_ROWS, 128), F32),
        scratch_shapes=[
            pltpu.VMEM((rows, 512), F32),
            pltpu.VMEM((rows, 512), BF16),
            pltpu.VMEM((rows, 512), BF16),
            pltpu.VMEM((GRAM_ROWS, 128), F32),
            pltpu.SemaphoreType.DMA((4,)),
        ] + sum_scratch(GRAM_ROWS // 512),
        compiler_params=pltpu.CompilerParams(
            collective_id=number, has_side_effects=True, vmem_limit_bytes=48 * 1024 * 1024
        ),
        name="gram_over_rows",
    )(snapshots)


def solve_kernel(row_total, gram_ref, start_ref, out_ref, gram):
    for at, (i, j) in enumerate(((0, 0), (0, 1), (1, 1))):
        for h in range(2):
            block = gram_ref[512 * at + 256 * h : 512 * at + 256 * h + 256, :] * (1.0 / row_total)
            gram[256 * i : 256 * i + 256, 256 * j + 128 * h : 256 * j + 128 * h + 128] = block
    gram[256:512, 0:256] = gram[0:256, 256:512].T
    parts = split3(gram[...])
    block, ratio = orth_rows(times(times(times(start_ref[...], parts), parts), parts))
    block, last_ratio = orth_rows(times(times(times(block, parts), parts), parts))
    block, error = corrected(block, block)
    out_ref[...] = block
    fine = jnp.logical_and(jnp.minimum(ratio, last_ratio) > 3e-6, error < 1e-5)

    @pl.when(jnp.logical_not(fine))
    def _():
        step_by_step(start_ref[...], parts, out_ref)


def group_solve(gram, start_block, row_total):
    return pl.pallas_call(
        functools.partial(solve_kernel, row_total),
        in_specs=[VMEM, VMEM],
        out_specs=VMEM,
        out_shape=jax.ShapeDtypeStruct((RANK, 512), F32),
        scratch_shapes=[pltpu.VMEM((512, 512), F32)],
        compiler_params=pltpu.CompilerParams(vmem_limit_bytes=16 * 1024 * 1024),
        name="group_solve",
    )(gram, start_block)


PIECES = 4


def merge_products(q, joined_ref, test_ref, first, second, third):
    part = test_ref.shape[0] // PIECES
    high, low = split(joined_ref[:, q * part : (q + 1) * part])
    test_high, test_low = split(test_ref[q * part : (q + 1) * part, :])
    one = bdot(high, high, NT)
    two = bdot(high, low, NT)
    three = bdot(high, test_high, NN) + bdot(high, test_low, NN) + bdot(low, test_high, NN)
    if q == 0:
        first[...], second[...], third[...] = one, two, three
    else:
        first[...] = first[...] + one
        second[...] = second[...] + two
        third[...] = third[...] + three


def basis_piece(high_low, x):
    high, low = split(x)
    both = bdot(high_low, high, NT)
    return both[:RANK] + both[RANK:] + bdot(high_low[:RANK], low, NT)


def merge_kernel(
    iterate_ref, x_hbm, test_ref, out_ref, merge_ref, x_ref, part_ref, first, second, third, x_sem, send_g, recv_g, *scratch
):
    g = lax.axis_index("grp")
    y, z, c = (lax.axis_index(name) for name in ROW)
    right, left = lax.rem(g + 1, 4), lax.rem(g + 3, 4)
    part = x_ref.shape[0] // PIECES
    x_pieces = pieces_in(x_hbm, x_ref, x_sem)
    work = StagedSum(part_ref, merge_ref, *scratch)
    peers = [(right, y, z, c), (left, y, z, c), work.mate] + [peer for _, peer in work.along_y + work.along_z]
    greet(peers)
    high_low = jnp.concatenate(split(iterate_ref[...]), axis=0)

    def place(block, q, first_row, size):
        return out_ref.at[rows_at(block * RANK + first_row, size), pl.ds(q * part, part)]

    def own(q):
        return [
            remote(place(g, q, 0, RANK), place(g, q, 0, RANK), send_g.at[k, q], recv_g.at[k, q], (peer, y, z, c))
            for k, peer in enumerate((right, left))
        ]

    def on(q):
        return [
            remote(place(block, q, at, 32), place(block, q, at, 32), send_g.at[k, q], recv_g.at[k, q], (peer, y, z, c))
            for k, block, at, peer in ((2, left, 0, right), (3, right, 32, left))
        ]

    owns, ons = [own(q) for q in range(PIECES)], [on(q) for q in range(PIECES)]

    def start(made):
        for one in made:
            one.start()

    def arrived(made):
        for one in made:
            one.wait_recv()

    def make(q):
        x_pieces[q].wait()
        out_ref[rows_at(g * RANK, RANK), q * part : (q + 1) * part] = basis_piece(
            high_low, x_ref[q * part : (q + 1) * part, :]
        )

    make(0)
    meet(peers)
    start(owns[0])
    make(1)
    start(owns[1])
    make(2)
    for q in range(PIECES):
        arrived(owns[q])
        start(ons[q])
        if q + 2 < PIECES:
            start(owns[q + 2])
        if q + 3 < PIECES:
            make(q + 3)
        if q > 0:
            arrived(ons[q - 1])
            merge_products(q - 1, out_ref, test_ref, first, second, third)
    arrived(ons[PIECES - 1])
    merge_products(PIECES - 1, out_ref, test_ref, first, second, third)
    merged = first[...] + second[...] + second[...].T
    for h in range(2):
        part_ref[256 * h : 256 * h + 256, :] = merged[:, 128 * h : 128 * h + 128]
    work.begin(0)
    part_ref[512:768, :] = third[...]
    part_ref[768:, :] = jnp.zeros((MERGE_ROWS - 768, 128), F32)
    work.begin(1)
    work.finish()
    for made in owns + ons:
        for one in made:
            one.wait_send()


def merged_over_rows(iterate, snapshots, test_block, number):
    rows = snapshots.shape[0]
    dma = pltpu.SemaphoreType.DMA
    return pl.pallas_call(
        merge_kernel,
        in_specs=[VMEM, pl.BlockSpec(memory_space=pl.ANY), VMEM],
        out_specs=[VMEM, VMEM],
        out_shape=[jax.ShapeDtypeStruct((4 * RANK, rows), F32), jax.ShapeDtypeStruct((MERGE_ROWS, 128), F32)],
        scratch_shapes=[
            pltpu.VMEM((rows, 512), F32),
            pltpu.VMEM((MERGE_ROWS, 128), F32),
            pltpu.VMEM((256, 256), F32),
            pltpu.VMEM((256, 256), F32),
            pltpu.VMEM((256, 128), F32),
            dma((PIECES,)),
            dma((4, PIECES)),
            dma((4, PIECES)),
        ] + sum_scratch(MERGE_ROWS // 512),
        compiler_params=pltpu.CompilerParams(
            collective_id=number, has_side_effects=True, vmem_limit_bytes=48 * 1024 * 1024
        ),
        name="merged_over_rows",
    )(iterate, snapshots, test_block)


def project_kernel(row_total, merge_ref, start_ref, joined_ref, out_ref, merged, coef_ref, factor):
    @pl.when(pl.program_id(0) == 0)
    def _():
        for h in range(2):
            merged[:, 128 * h : 128 * h + 128] = merge_ref[256 * h : 256 * h + 256, :] * (1.0 / row_total)
        parts = split3(merged[...])

        def to_modes(block):
            inverse, _, _ = lower_inverse(fdot(times(block, parts), block, NT))
            block = fdot(inverse, block)
            return corrected(block, times(block, parts))

        block, ratio = orth_rows(times(times(start_ref[...], parts), parts))
        block, next_ratio = orth_rows(times(times(block, parts), parts))
        coef, error = to_modes(times(times(block, parts), parts))
        coef_ref[...] = coef
        fine = jnp.logical_and(jnp.minimum(ratio, next_ratio) > 3e-6, error < 1e-4)

        @pl.when(jnp.logical_not(fine))
        def _():
            step_by_step(start_ref[...], parts, coef_ref)
            coef_ref[...] = to_modes(coef_ref[...])[0]

        coef = coef_ref[...]
        test_coeffs = fdot(coef, merge_ref[512:768, :]) * (1.0 / row_total)
        high, low = split(fdot(test_coeffs, coef, TN))
        factor[0:128, :] = high
        factor[128:, :] = low

    size = out_ref.shape[0]
    here = pl.ds(pl.multiple_of(pl.program_id(0) * size, 128), size)
    high, low = split(joined_ref[:, here])
    both = bdot(factor[...], high, NN)
    out_ref[...] = (both[:128] + both[128:] + bdot(factor[0:128, :], low, NN)).T


def project(merge, start_merge, joined, row_total):
    rows = joined.shape[1]
    return pl.pallas_call(
        functools.partial(project_kernel, row_total),
        grid=(rows // 896,),
        in_specs=[VMEM, VMEM, VMEM],
        out_specs=pl.BlockSpec((896, 128), lambda i: (i, 0)),
        out_shape=jax.ShapeDtypeStruct((rows, 128), F32),
        scratch_shapes=[pltpu.VMEM((256, 256), F32), pltpu.VMEM((RANK, 256), F32), pltpu.VMEM((256, 256), BF16)],
        compiler_params=pltpu.CompilerParams(vmem_limit_bytes=16 * 1024 * 1024),
        name="project",
    )(merge, start_merge, joined)


def on_device(snapshots, test_block, start_block, start_merge):
    row_total = snapshots.shape[0] * 64
    gram = gram_over_rows(snapshots, 0)
    iterate = group_solve(gram, start_block.T, row_total)
    joined, merge = merged_over_rows(iterate, snapshots, test_block, 1)
    return project(merge, start_merge.T, joined, row_total)


def solution(mesh):
    finer = Mesh(
        mesh.devices.reshape(mesh.shape["grp"], 4, 8, 2), ("grp", "row_0", "row_1", "row_2")
    )
    placed = (P(ROW, "grp"), P(ROW, "grp"), P("grp", None), P())
    return jax.shard_map(
        on_device, mesh=finer, in_specs=placed, out_specs=P(ROW, "grp"), check_vma=False
    )
```
